32 devices in a mesh: gx: 4 (over x, core), gy: 4 (over z), gz: 2 (over y).
Axes of the slice: x: 2, y: 2, z: 4, core: 2. Of those that a mesh axis runs over, the one named last changes fastest.
Arguments:
- fine_coef: bfloat16 [256, 512], P(('gx', 'gy', 'gz')), may hold values from -6 to 6
- mid_leaf: bfloat16 [32, 512], P(('gx', 'gy', 'gz')), may hold values from -6 to 6
- mid_child: int32 [32, 8], P(('gx', 'gy', 'gz')), may hold values from 0 to 7, as said below
- mid_parent: int32 [32], P(('gx', 'gy', 'gz')), may hold values from 0 to 31, each once
- mid_refined: int32 [32], P(('gx', 'gy', 'gz')), may hold values 0 or 1
- fine_nbr: int32 [256, 27], P(('gx', 'gy', 'gz')), may hold values from -1 to 255, as said below
- mid_nbr: int32 [32, 27], P(('gx', 'gy', 'gz')), may hold values from -1 to 31, as said below
- coarse_nbr: int32 [4, 27], replicated, may hold values from -1 to 3, as said below
- op_factor: float32 [3, 32, 3, 8, 8], replicated, may hold values from -1 to 1
- term_weight: float32 [32], replicated, may hold values from 0.05 to 1
Outputs:
- fine_out: float32 [256, 512], P(('gx', 'gy', 'gz'))
- mid_out: float32 [32, 512], P(('gx', 'gy', 'gz'))
The draws below stay inside these ranges and needn't reach their ends.
Inputs may be any that keep to these rules, and one draw needn't show every extreme that they name: `fine_nbr`: column d names the fine box adjacent across displacement (d // 9 - 1, d // 3 % 3 - 1, d % 3 - 1), or -1. Column 13 is the row's own box. Box g lies on device g // 8; the named box's device differs from the row's device along each of gx, gy, gz by 0 or by that component of the displacement. `mid_nbr`: column d names the middle box adjacent across displacement (d // 9 - 1, d // 3 % 3 - 1, d % 3 - 1), or -1. Column 13 is the row's own box. Box g lies on device g; the named box's device differs from the row's device along each of gx, gy, gz by 0 or by that component of the displacement. `coarse_nbr`: column d names the coarse box adjacent across displacement (d // 9 - 1, d // 3 % 3 - 1, d % 3 - 1), or -1. Column 13 is the row's own box. `mid_child`: the 1 row of one device together name each of its 8 local fine slots exactly once. `mid_parent`: each value appears once.
All inputs are finite; a program needn't handle non-finite values. No bound on the sum of `mid_refined` on one device may be relied on, other than what follows from the above.
Results may differ from the reference program's by a relative error of at most 0.006.
Values may be sent and summed in bfloat16 or wider, within the bound.
A program may use at most 64 MiB of HBM per device.

```python
import math
import jax
import jax.numpy as jnp
import numpy as np
from jax import lax

K = 8
TERMS = 32
MB_DEV = 1
FINE = 256
MID = 32
COARSE = 4
N_GX = 4
N_GY = 4
N_GZ = 2
DEVICES = 32


def near_boxes(key, per_device):
    box_total = per_device * DEVICES
    box_index = jnp.arange(box_total, dtype=jnp.int32)
    device = box_index // per_device
    coord_x = device // (N_GY * N_GZ)
    coord_y = device // N_GZ % N_GY
    coord_z = device % N_GZ
    column = jnp.arange(27, dtype=jnp.int32)
    step_x = column // 9 - 1
    step_y = column // 3 % 3 - 1
    step_z = column % 3 - 1
    key_hop, key_slot, key_gone = jax.random.split(key, 3)
    hop_bits = jax.random.randint(key_hop, (box_total, 3, 27), 0, 2, dtype=jnp.int32)
    near_x = coord_x[:, None] + step_x[None, :] * hop_bits[:, 0]
    near_y = coord_y[:, None] + step_y[None, :] * hop_bits[:, 1]
    near_z = coord_z[:, None] + step_z[None, :] * hop_bits[:, 2]
    inside = (near_x >= 0) & (near_x < N_GX) & (near_y >= 0) & (near_y < N_GY) & (near_z >= 0) & (near_z < N_GZ)
    slot_pick = jax.random.randint(key_slot, (box_total, 27), 0, per_device, dtype=jnp.int32)
    gone_mask = jax.random.randint(key_gone, (box_total, 27), 0, 5, dtype=jnp.int32) == 0
    named_box = ((near_x * N_GY + near_y) * N_GZ + near_z) * per_device + slot_pick
    result = jnp.where(inside & jnp.logical_not(gone_mask), named_box, -1)
    result = jnp.where(column[None, :] == 13, box_index[:, None], result)
    return result.astype(jnp.int32)


def draw_fine_nbr(key, part):
    return near_boxes(jax.random.fold_in(key, 11), 8 * MB_DEV)


def draw_mid_nbr(key, part):
    return near_boxes(jax.random.fold_in(key, 12), MB_DEV)


def draw_coarse_nbr(key, part):
    key_pick, key_gone = jax.random.split(jax.random.fold_in(key, 13), 2)
    column = jnp.arange(27, dtype=jnp.int32)
    box_index = jnp.arange(COARSE, dtype=jnp.int32)
    picked = jax.random.randint(key_pick, (COARSE, 27), 0, COARSE, dtype=jnp.int32)
    gone_mask = jax.random.randint(key_gone, (COARSE, 27), 0, 5, dtype=jnp.int32) == 0
    result = jnp.where(gone_mask, -1, picked)
    result = jnp.where(column[None, :] == 13, box_index[:, None], result)
    return result.astype(jnp.int32)


def shuffle_slots(single_key):
    return jax.random.permutation(single_key, 8 * MB_DEV)


def draw_mid_child(key, part):
    all_keys = jax.random.split(jax.random.fold_in(key, 14), DEVICES)
    orders = jax.vmap(shuffle_slots)(all_keys)
    return orders.reshape(MID, 8).astype(jnp.int32)


def place_ends(entries, key, low, top_value):
    index_at = [jax.random.randint(jax.random.fold_in(key, axis), (), 0, length) for axis, length in enumerate(entries.shape)]
    longest = entries.shape.index(max(entries.shape))
    next_to = index_at[:longest] + [(index_at[longest] + 1) % entries.shape[longest]] + index_at[longest + 1:]
    return entries.at[tuple(index_at)].set(low).at[tuple(next_to)].set(top_value)


def steps_of(rng, extent, shards, low, high):
    def one(axis_at, shards_of):
        draws = jax.random.uniform(jax.random.fold_in(jax.random.fold_in(rng, 6), axis_at), (shards_of,), jnp.float32, low / len(shards), high / len(shards))
        return jnp.repeat(jnp.exp(draws), extent[axis_at] // shards_of).reshape((-1,) + (1,) * (len(extent) - axis_at - 1))

    level = one(*shards[0])
    for cut in shards[1:]:
        level = level * one(*cut)
    return level


def normal_values(key, shape, scale, reach, cuts=(), held_as=jnp.bfloat16):
    array = jax.random.normal(key, shape, jnp.float32) * scale
    if len(cuts) > 0:
        array = steps_of(key, shape, cuts, -0.22, 0.18) * array
    return jnp.clip(array, min=-reach, max=reach).astype(held_as)


def setup_inputs(seed: int = 0) -> dict:
    keys = jax.random.split(jax.random.key(seed), 11)
    fine_coef = normal_values(keys[0], (FINE, K ** 3), 1.0, 6.0, ((0, 32),))
    mid_leaf = normal_values(keys[1], (MID, K ** 3), 1.0, 6.0, ((0, 32),))
    mid_child = draw_mid_child(jax.random.fold_in(keys[10], 71), 0)
    mid_parent = jax.random.permutation(keys[3], MID).astype(jnp.int32)
    mid_refined = place_ends((jax.random.randint(keys[4], (MID,), 0, 3) < 2).astype(jnp.int32), jax.random.fold_in(keys[4], 1), 0, 1)
    fine_nbr = draw_fine_nbr(jax.random.fold_in(keys[10], 71), 0)
    mid_nbr = draw_mid_nbr(jax.random.fold_in(keys[10], 71), 0)
    coarse_nbr = draw_coarse_nbr(jax.random.fold_in(keys[10], 71), 0)
    op_factor = normal_values(keys[8], (3, TERMS, 3, K, K), 0.16, 1.0, (), jnp.float32)
    term_weight = jnp.clip(jnp.exp(jax.random.uniform(keys[9], (TERMS,), jnp.float32, math.log(0.05), math.log(1.0))), 0.05, 1.0)
    return dict(fine_coef=fine_coef, mid_leaf=mid_leaf, mid_child=mid_child, mid_parent=mid_parent, mid_refined=mid_refined, fine_nbr=fine_nbr, mid_nbr=mid_nbr, coarse_nbr=coarse_nbr, op_factor=op_factor, term_weight=term_weight)


exact_mode = lax.Precision.HIGHEST

def poly_multiply(left, right):
    result = [0.0] * (len(left) + len(right) - 1)
    for first, left_coef in enumerate(left):
        for second, right_coef in enumerate(right):
            result[first + second] += left_coef * right_coef
    return result

def poly_compose(coeffs, factor, offset):
    result = [0.0]
    power_term = [1.0]
    for coef in coeffs:
        padded = result + [0.0] * (len(power_term) - len(result))
        result = [padded[place] + coef * power_term[place] for place in range(len(power_term))]
        power_term = poly_multiply(power_term, [offset, factor])
    return result

def legendre_table(basis_order):
    polys = [[1.0], [0.0, 1.0]]
    for degree in range(1, basis_order):
        upper = [0.0] + [(2 * degree + 1) * coef for coef in polys[degree]]
        lower = [degree * coef for coef in polys[degree - 1]] + [0.0] * (len(upper) - len(polys[degree - 1]))
        polys.append([(upper[place] - lower[place]) / (degree + 1) for place in range(len(upper))])
    return [[math.sqrt(2 * degree + 1) * coef for coef in poly_compose(polys[degree], 2.0, -1.0)] for degree in range(basis_order)]

def two_scale(basis_order):
    shifted = legendre_table(basis_order)
    filters = np.zeros((2, basis_order, basis_order))
    for which_half in range(2):
        for row_at in range(basis_order):
            halved = poly_compose(shifted[row_at], 0.5, 0.5 * which_half)
            for col_at in range(basis_order):
                product = poly_multiply(halved, shifted[col_at])
                total = sum((coef / (place + 1) for place, coef in enumerate(product)))
                filters[which_half, row_at, col_at] = total / math.sqrt(2.0)
    return jnp.asarray(filters, jnp.float32)

def compress(children, filters):
    box_count = children.shape[0]
    basis_order = filters.shape[1]
    cube_form = children.reshape(box_count, 2, 2, 2, basis_order, basis_order, basis_order)
    section_one = jnp.einsum('bijlxyz,ipx->bjlpyz', cube_form, filters, precision=exact_mode)
    section_two = jnp.einsum('bjlpyz,jqy->blpqz', section_one, filters, precision=exact_mode)
    section_three = jnp.einsum('blpqz,lrz->bpqr', section_two, filters, precision=exact_mode)
    return section_three.reshape(box_count, basis_order ** 3)

def prolong(parents, filters):
    box_count = parents.shape[0]
    basis_order = filters.shape[1]
    cube_form = parents.reshape(box_count, basis_order, basis_order, basis_order)
    section_one = jnp.einsum('bpqr,ipx->bixqr', cube_form, filters, precision=exact_mode)
    section_two = jnp.einsum('bixqr,jqy->bijxyr', section_one, filters, precision=exact_mode)
    section_three = jnp.einsum('bijxyr,lrz->bijlxyz', section_two, filters, precision=exact_mode)
    return section_three.reshape(box_count, 8, basis_order ** 3)

def level_tables(factors, weights):
    basis_order = factors.shape[-1]
    term_count = factors.shape[0]
    across = jnp.transpose(factors, (1, 0, 3, 2))
    blocks = weights[None, None, :, None, None, None, None] * across[:, None, :, :, None, :, None] * across[None, :, :, None, :, None, :]
    blocks = blocks.reshape(3, 3, term_count * basis_order * basis_order, basis_order * basis_order)
    return (factors.astype(jnp.bfloat16), blocks.astype(jnp.bfloat16))

def apply_boxes(sources, factor_bf, blocks):
    box_count = sources.shape[0]
    basis_order = factor_bf.shape[-1]
    plane_size = basis_order * basis_order
    cube_form = sources.reshape(box_count, 3, 3, 3, basis_order, plane_size)
    running = jnp.zeros((box_count * basis_order, plane_size), jnp.float32)
    for along_y in range(3):
        for along_z in range(3):
            picked = cube_form[:, :, along_y, along_z]
            mixed_terms = jnp.einsum('mdax,bdxq->bamq', factor_bf.astype(jnp.float32), picked.astype(jnp.float32), precision=exact_mode).astype(jnp.bfloat16)
            flat_terms = mixed_terms.reshape(box_count * basis_order, -1)
            running = running + jnp.dot(flat_terms.astype(jnp.float32), blocks[along_y, along_z].astype(jnp.float32), precision=exact_mode)
    return running.reshape(box_count, basis_order ** 3)

def apply_level(source_table, near_ids, factors, weights):
    factor_bf, blocks = level_tables(factors, weights)
    total_rows = near_ids.shape[0]
    block_rows = math.gcd(total_rows, 128)
    grouped = near_ids.reshape(total_rows // block_rows, block_rows, 27)

    def one_block(some_rows):
        sources = source_table[jnp.maximum(some_rows, 0)] * (some_rows >= 0)[:, :, None].astype(source_table.dtype)
        return apply_boxes(sources, factor_bf, blocks)
    return lax.map(one_block, grouped).reshape(total_rows, -1)

def reference(fine_coef, mid_leaf, mid_child, mid_parent, mid_refined, fine_nbr, mid_nbr, coarse_nbr, op_factor, term_weight):
    filters = two_scale(K)
    slots_dev = 8 * MB_DEV
    mid_count = mid_child.shape[0]
    volume = fine_coef.shape[1]
    owner_dev = jnp.arange(mid_count, dtype=jnp.int32) // MB_DEV
    child_rows = (owner_dev[:, None] * slots_dev + mid_child).astype(jnp.int32)
    flat_rows = child_rows.reshape(-1)
    refined = mid_refined.astype(jnp.float32)
    live_mask = jnp.zeros((FINE,), jnp.float32).at[flat_rows].set(jnp.repeat(refined, 8))
    children = fine_coef[child_rows].astype(jnp.float32)
    compressed = compress(children, filters)
    mid_source = jnp.where(mid_refined[:, None] > 0, compressed, mid_leaf.astype(jnp.float32)).astype(jnp.bfloat16)
    mid_float = mid_source.astype(jnp.float32)
    spread = prolong(mid_float, filters)
    fine_from = jnp.zeros((FINE, volume), jnp.float32).at[flat_rows].set(spread.reshape(-1, volume))
    fine_detail = (live_mask[:, None] * (fine_coef.astype(jnp.float32) - fine_from)).astype(jnp.bfloat16)
    parent = (mid_parent // 8).astype(jnp.int32)
    octant = mid_parent % 8
    octant_hot = (octant[:, None] == jnp.arange(8, dtype=jnp.int32)[None, :]).astype(jnp.float32)
    placed = octant_hot[:, :, None] * mid_float[:, None, :]
    coarse_source = jnp.zeros((COARSE, volume), jnp.float32).at[parent].add(compress(placed, filters))
    parent_source = coarse_source[parent]
    from_coarse = lax.optimization_barrier(jnp.sum(octant_hot[:, :, None] * prolong(parent_source, filters), axis=1))
    mid_detail = (mid_float - from_coarse).astype(jnp.bfloat16)
    coarse_table = coarse_source.astype(jnp.bfloat16)
    coarse_output = apply_level(coarse_table, coarse_nbr, op_factor[2], term_weight)
    parent_out = coarse_output[parent]
    mid_out = apply_level(mid_detail, mid_nbr, op_factor[1], term_weight) + lax.optimization_barrier(jnp.sum(octant_hot[:, :, None] * prolong(parent_out, filters), axis=1))
    fine_back = jnp.zeros((FINE, volume), jnp.float32).at[flat_rows].set(prolong(mid_out, filters).reshape(-1, volume))
    fine_out = live_mask[:, None] * (apply_level(fine_detail, fine_nbr, op_factor[0], term_weight) + fine_back)
    return (fine_out, mid_out)
```

```python
import math

import jax
import jax.numpy as jnp
import numpy as np
from jax import lax
from jax.experimental import pallas as pl
from jax.experimental.pallas import tpu as pltpu
from jax.sharding import PartitionSpec as P

MESH = pl.DeviceIdType.MESH
AXES = ("gx", "gy", "gz")
CENTRE = 13
QUAD = 4
F32 = jnp.float32
BF16 = jnp.bfloat16


def poly_multiply(left, right):
    result = [0.0] * (len(left) + len(right) - 1)
    for first, left_coef in enumerate(left):
        for second, right_coef in enumerate(right):
            result[first + second] += left_coef * right_coef
    return result


def poly_compose(coeffs, factor, offset):
    result = [0.0]
    power_term = [1.0]
    for coef in coeffs:
        padded = result + [0.0] * (len(power_term) - len(result))
        result = [padded[place] + coef * power_term[place] for place in range(len(power_term))]
        power_term = poly_multiply(power_term, [offset, factor])
    return result


def legendre_table(basis_order):
    polys = [[1.0], [0.0, 1.0]]
    for degree in range(1, basis_order):
        upper = [0.0] + [(2 * degree + 1) * coef for coef in polys[degree]]
        lower = [degree * coef for coef in polys[degree - 1]] + [0.0] * (
            len(upper) - len(polys[degree - 1])
        )
        polys.append([(upper[place] - lower[place]) / (degree + 1) for place in range(len(upper))])
    return [
        [math.sqrt(2 * degree + 1) * coef for coef in poly_compose(polys[degree], 2.0, -1.0)]
        for degree in range(basis_order)
    ]


def two_scale(basis_order):
    shifted = legendre_table(basis_order)
    filters = np.zeros((2, basis_order, basis_order))
    for which_half in range(2):
        for row_at in range(basis_order):
            halved = poly_compose(shifted[row_at], 0.5, 0.5 * which_half)
            for col_at in range(basis_order):
                product = poly_multiply(halved, shifted[col_at])
                total = sum((coef / (place + 1) for place, coef in enumerate(product)))
                filters[which_half, row_at, col_at] = total / math.sqrt(2.0)
    return np.asarray(filters, np.float32)


def halves(array):
    high = array.astype(BF16)
    return high, (array - high.astype(array.dtype)).astype(BF16)


def np_halves(array):
    array = np.asarray(array, np.float32)
    high = array.astype(BF16)
    return high, (array - high.astype(np.float32)).astype(BF16)


def dot(left, right):
    return jnp.dot(left, right, preferred_element_type=F32)


def dot_rows(left, right):
    return lax.dot_general(left, right, (((1,), (1,)), ((), ())), preferred_element_type=F32)


def constants(terms, devices, batch):
    filters = two_scale(8)
    table = {}
    row = np.arange(8 * terms)
    lane = np.arange(64 * terms)
    same = (row % terms)[:, None] == (lane // 64)[None, :]
    spread = [same & ((row // terms)[:, None] == part[None, :]) for part in (lane // 8 % 8, lane % 8)]
    table["spread"] = np.concatenate(spread, axis=1).astype(BF16)
    swap = (row // 8)[:, None] == (row % terms)[None, :]
    swap &= (row % 8)[:, None] == (row // terms)[None, :]
    table["swap"] = swap.astype(BF16)
    table["widen"] = (np.arange(72)[:, None] == (np.arange(192) // 8)[None, :]).astype(BF16)
    plane = np.einsum("jqy,lrz->jlyzqr", filters, filters)
    table["gather_plane"] = np.concatenate(np_halves(plane.reshape(256, 64)), axis=1)
    plane = np.einsum("jqy,lrz->qrjlyz", filters, filters)
    table["scatter_plane"] = np.concatenate(np_halves(plane.reshape(64, 256)), axis=1)
    parts = [np.asarray(part, np.float32) for part in np_halves(filters)]
    both = np.stack(parts, axis=1).reshape(4, 8, 8)
    flip = np.swapaxes(both, 1, 2)
    table["child_in"] = np.repeat(both, 8, axis=2)
    table["child_out"] = np.tile(np.repeat(flip, 8, axis=1), (1, 1, 4))
    table["mid_in"] = np.tile(both, (1, 1, devices))
    table["mid_out"] = np.tile(flip, (1, 1, batch * 4))
    own = [np.concatenate([flip[2 * i], flip[2 * i], flip[2 * i + 1]], axis=1) for i in range(2)]
    table["own_out"] = np.stack(own)
    cell = np.arange(27 * 8) // 8
    cells = np.zeros((8, 27 * 8), np.int32)
    cells[:4] = np.stack([cell // 9 - 1, cell // 3 % 3 - 1, cell % 3 - 1, np.arange(27 * 8) % 8])
    table["cells"] = cells
    return table


def kernel(sizes, names, batch, levels, terms, coarse, args, consts, outs, scratch):
    size_x, size_y, size_z = sizes
    devices = size_x * size_y * size_z
    here = [lax.axis_index(axis) for axis in AXES]
    me = (here[0] * size_y + here[1]) * size_z + here[2]
    fine_ref, mid_ref = outs
    (loaded, held, halo, rows, factor_left, factor_right, tables, mixers, mixers_t, block_mix, picks, coarse_tab,
     load_sem, held_sem, row_send, row_recv, halo_send, halo_recv) = scratch

    def place_of(device):
        return (device // (size_y * size_z), device // size_z % size_y, device % size_z)

    def each_peer(body):
        if devices <= 64:
            for offset in range(1, devices):
                body(lax.rem(me + offset, devices))
        else:
            def step(offset, carry):
                body(lax.rem(me + offset, devices))
                return carry
            lax.fori_loop(1, devices, step, 0)

    barrier = pltpu.get_barrier_semaphore()
    each_peer(lambda peer: pl.semaphore_signal(
        barrier, inc=1, device_id=place_of(peer), device_id_type=MESH))

    loads = {}
    for at, (name, source) in enumerate(args.items()):
        loads[name] = pltpu.make_async_copy(source, loaded[name], load_sem.at[at])
    for at, (name, source) in enumerate(consts.items()):
        loads[name] = pltpu.make_async_copy(source, held[name], held_sem.at[at])
    order = ["mid_child", "mid_parent", "mid_refined", "fine_coef", "mid_leaf", "child_in", "gather_plane",
             "child_out", "scatter_plane"]
    order += [name for name in loads if name not in order]
    for name in order:
        loads[name].start()

    def ready(*wanted):
        for name in wanted:
            loads[name].wait()

    ready("mid_child", "mid_parent", "mid_refined", "fine_coef", "mid_leaf", "child_in", "gather_plane")
    child = [loaded["mid_child"][0, o] for o in range(8)]
    refined = loaded["mid_refined"][0] > 0
    live = jnp.where(refined, 1.0, 0.0).astype(F32)
    mid_parent = loaded["mid_parent"][0]
    my_parent = lax.shift_right_logical(mid_parent, 3)
    my_octant = mid_parent & 7
    flat = loaded["fine_coef"][...].astype(F32)
    by_row = jnp.concatenate([flat[:, 64 * x : 64 * x + 64] for x in range(8)], axis=0)
    slot_lane = lax.broadcasted_iota(jnp.int32, (8, 64), 1) & 7
    child_in = [held["child_in"][k] for k in range(4)]
    blocks = []
    for part in range(2):
        for jl in range(4):
            block = jnp.where(slot_lane == child[jl], child_in[part], 0.0)
            blocks.append(block + jnp.where(slot_lane == child[4 + jl], child_in[2 + part], 0.0))
    mixed = dot(jnp.concatenate(blocks, axis=0).astype(BF16), by_row.astype(BF16))
    mixed = mixed[:32] + mixed[32:]

    def stack_halves(array):
        high, low = halves(array)
        return jnp.concatenate([high.astype(F32), low.astype(F32)], axis=0).astype(BF16)

    def close_children(mixed, boxes):
        wide = [
            jnp.concatenate([mixed[(4 * k + jl) * 8 : (4 * k + jl) * 8 + 8] for jl in range(4)], axis=1)
            for k in range(boxes)
        ]
        wide = wide[0] if boxes == 1 else jnp.concatenate(wide, axis=0)
        got = dot(stack_halves(wide), held["gather_plane"][...])
        count = boxes * 8
        return got[:count, :64] + got[:count, 64:] + got[count:, :64]

    def open_plane(block, exact=False):
        count = block.shape[0]
        if exact:
            got = dot(block.astype(BF16), held["scatter_plane"][...])
            return got[:, :256] + got[:, 256:]
        got = dot(stack_halves(block), held["scatter_plane"][...])
        return got[:count, :256] + got[:count, 256:] + got[count:, :256]

    def lanes_to_rows(plane):
        count = plane.shape[0] // 8
        return jnp.concatenate(
            [plane[8 * k : 8 * k + 8, 64 * jl : 64 * jl + 64] for k in range(count) for jl in range(4)], axis=0
        )

    def triple(rows_f32):
        high, low = halves(rows_f32)
        high, low = high.astype(F32), low.astype(F32)
        return jnp.concatenate([high, low, high], axis=0).astype(BF16)

    compressed = close_children(mixed, 1)
    leaf = jnp.broadcast_to(loaded["mid_leaf"][...].astype(F32), (8, 512))
    block_lane = lax.shift_right_logical(lax.broadcasted_iota(jnp.int32, (8, 512), 1), 6)
    leaf = jnp.where(block_lane == lax.broadcasted_iota(jnp.int32, (8, 512), 0), leaf, 0.0)
    leaf_square = leaf[:, :64]
    for x in range(1, 8):
        leaf_square = leaf_square + leaf[:, 64 * x : 64 * x + 64]
    mid_source = jnp.where(refined, compressed, leaf_square).astype(BF16).astype(F32)
    note = lax.broadcasted_iota(jnp.int32, (8, 64), 1)
    place = jnp.where(note == 0, my_parent + 1, jnp.where(note == 1, my_octant, 0)).astype(F32)
    rows[me] = jnp.concatenate([mid_source, place], axis=1).astype(BF16)

    ready("child_out", "scatter_plane")
    jl_lane = lax.shift_right_logical(lax.broadcasted_iota(jnp.int32, (64, 32), 1), 3)
    slot_row = lax.broadcasted_iota(jnp.int32, (64, 32), 0) & 7

    def child_lane(i):
        return jnp.where(jl_lane == 0, child[4 * i],
                         jnp.where(jl_lane == 1, child[4 * i + 1],
                                   jnp.where(jl_lane == 2, child[4 * i + 2], child[4 * i + 3])))

    chosen = [slot_row == child_lane(i) for i in range(2)]
    out_parts = [
        jnp.where(chosen[0], held["child_out"][part], 0.0)
        + jnp.where(chosen[1], held["child_out"][2 + part], 0.0)
        for part in range(2)
    ]
    child_out = jnp.concatenate([out_parts[0], out_parts[0], out_parts[1]], axis=1).astype(BF16)

    def to_children(plane):
        return dot(child_out, triple(lanes_to_rows(plane)))

    detail = live * (by_row - to_children(open_plane(mid_source, exact=True)))
    detail = jnp.concatenate([detail[8 * x : 8 * x + 8] for x in range(8)], axis=1)
    halo[CENTRE] = detail.astype(BF16)

    steps = [(c // 9 - 1, c // 3 % 3 - 1, c % 3 - 1) for c in range(27)]

    def inside(step):
        tests = []
        for at, size, move in zip(here, sizes, step):
            if move == 1:
                tests.append(at < size - 1)
            elif move == -1:
                tests.append(at > 0)
        found = tests[0]
        for test in tests[1:]:
            found = found & test
        return found

    def halo_copy(cell):
        move = steps[cell]
        peer = tuple(at + part for at, part in zip(here, move))
        return pltpu.make_async_remote_copy(
            src_ref=halo.at[CENTRE],
            dst_ref=halo.at[26 - cell],
            send_sem=halo_send.at[cell],
            recv_sem=halo_recv.at[26 - cell],
            device_id=peer,
            device_id_type=MESH,
        )

    others = [cell for cell in range(27) if cell != CENTRE]
    pl.semaphore_wait(barrier, devices - 1)
    each_peer(lambda peer: pltpu.make_async_remote_copy(
        src_ref=rows.at[me],
        dst_ref=rows.at[me],
        send_sem=row_send.at[0],
        recv_sem=row_recv.at[0],
        device_id=place_of(peer),
        device_id_type=MESH,
    ).start())
    for cell in others:
        @pl.when(inside(steps[cell]))
        def _(cell=cell):
            halo_copy(cell).start()

        @pl.when(jnp.logical_not(inside(steps[cell])))
        def _(cell=cell):
            halo[cell] = jnp.zeros(halo.shape[1:], BF16)

    ready("op_factor", "term_weight", "spread", "swap", "widen")
    factor = loaded["op_factor"]
    planes = []
    for level in range(levels):
        for e in range(3):
            planes.append(jnp.concatenate([factor[level, e, b] for b in range(8)], axis=1))
    plane = jnp.concatenate(planes, axis=0)
    weight = jnp.concatenate([loaded["term_weight"][...]] * 8, axis=1)
    rounded = plane.astype(BF16)
    left_side = stack_halves(plane * weight)
    right_side = stack_halves(plane)
    count = plane.shape[0]
    width = 64 * terms
    for at in range(0, width, 512):
        got = dot(left_side, held["spread"][:, at : at + 512])
        got = got[:count] + got[count:]
        factor_left[:, :, at : at + 512] = got.reshape(levels * 3, 8, 512)
        got = dot(right_side, held["spread"][:, width + at : width + at + 512])
        got = got[:count] + got[count:]
        factor_right[:, :, at : at + 512] = got.reshape(levels * 3, 8, 512)
    turned = dot_rows(held["swap"][...], rounded).astype(BF16)
    mixers[...] = turned
    mixers_t[...] = dot(turned, held["widen"][...])

    def table_step(at, carry):
        level, ey = at // 3, at % 3
        left = factor_left.at[at]
        for ez in range(3):
            right = factor_right[level * 3 + ez]
            base = (ey * 3 + ez) * 64
            for k in range(4):
                pair = [left[2 * k + half : 2 * k + half + 1, :] * right for half in range(2)]
                start = pl.multiple_of(base + 16 * k, 16)
                tables[level, pl.ds(start, 16), :] = jnp.concatenate(pair, axis=0).astype(BF16)
        return carry

    lax.fori_loop(0, levels * 3, table_step, 0)
    own_lane = (lax.broadcasted_iota(jnp.int32, (8, 192), 1) & 7) == lax.broadcasted_iota(jnp.int32, (8, 192), 0)

    def mix_step(at, carry):
        some = mixers_t[pl.ds(pl.multiple_of(at * 16, 16), 16), :]
        some = jnp.where(own_lane[None], jnp.broadcast_to(some[:, None, :], (16, 8, 192)), 0.0)
        block_mix[pl.ds(pl.multiple_of(at * 128, 128), 128), :] = some.reshape(128, 192).astype(BF16)
        return carry

    lax.fori_loop(0, terms // 2, mix_step, 0)

    ready("cells", "fine_nbr")
    cells = held["cells"]
    spot = [here[k] + cells[k : k + 1, :] for k in range(3)]
    there = None
    for k in range(3):
        test = (spot[k] >= 0) & (spot[k] < sizes[k])
        there = test if there is None else there & test
    names_row = ((spot[0] * size_y + spot[1]) * size_z + spot[2]) * 8 + cells[3:4, :]
    names_row = jnp.where(there, names_row, -2)
    near = loaded["fine_nbr"][...]
    hot = [(near[:, d : d + 1] == names_row).astype(F32) for d in range(27)]
    picks[...] = jnp.concatenate(hot, axis=0).astype(BF16)

    ready("mid_in", "mid_out", "own_out", "mid_nbr", "coarse_nbr")
    all_rows = rows.at[pl.ds(0, devices - 1)]
    pltpu.make_async_copy(all_rows, all_rows, row_recv.at[0]).wait()
    gathered = rows[...].astype(F32).reshape(devices * 8, 128).astype(BF16)
    reader_lane = lax.broadcasted_iota(jnp.int32, (8, 128), 1)
    reader = jnp.where(reader_lane == 64, 8.0, jnp.where(reader_lane == 65, 1.0, 0.0)).astype(BF16)
    code = dot_rows(reader, gathered) - 8.0
    near_rows = []
    for d in range(27):
        named = loaded["mid_nbr"][0, d]
        got = rows[jnp.maximum(named, 0)].astype(F32)
        near_rows.append(jnp.where(named >= 0, got, 0.0))
    near_rows = jnp.concatenate(near_rows, axis=0)
    near_code = near_rows[:, 64:65] * 8.0 + near_rows[:, 65:66] - 8.0
    batch_lane = lax.broadcasted_iota(jnp.int32, (8, batch * 32), 1)
    batch_code = lax.shift_right_logical(batch_lane, 5) * 8 + (lax.shift_right_logical(batch_lane, 3) & 3)

    def coarse_step(at, total):
        first = at * (batch * 8)
        first_f = first.astype(F32) if hasattr(first, "astype") else float(first)
        blocks = []
        for part in range(2):
            for k in range(batch):
                for jl in range(4):
                    want = first_f + float(8 * k + jl)
                    block = jnp.where(code == want, held["mid_in"][part], 0.0)
                    blocks.append(block + jnp.where(code == want + 4.0, held["mid_in"][2 + part], 0.0))
        mixed = dot(jnp.concatenate(blocks, axis=0).astype(BF16), gathered)
        half = batch * 32
        source = close_children(mixed[:half, :64] + mixed[half:, :64], batch)
        held_source = source.astype(BF16).astype(F32)
        double = jnp.concatenate([held_source, held_source], axis=1)
        coarse_tab[pl.ds(at * batch, batch)] = double.reshape(batch, 8, 128)
        lane_code = first_f + batch_code.astype(F32)
        parts = [[], []]
        for d in range(27):
            mine = near_code[8 * d : 8 * d + 8]
            lower, upper = mine == lane_code, mine == lane_code + 4.0
            for part in range(2):
                block = jnp.where(lower, held["mid_out"][part], 0.0)
                parts[part].append(block + jnp.where(upper, held["mid_out"][2 + part], 0.0))
        parts = [jnp.concatenate(part, axis=0).astype(BF16) for part in parts]
        spread = triple(lanes_to_rows(open_plane(source)))
        rows_out = dot(jnp.concatenate([parts[0], parts[0], parts[1]], axis=1), spread)
        return total + rows_out

    batches = coarse // batch
    zero = jnp.zeros((216, 64), F32)
    from_coarse = coarse_step(0, zero) if batches == 1 else lax.fori_loop(0, batches, coarse_step, zero)
    mid_detail = near_rows[:, :64] - from_coarse
    mid_blocks = [
        jnp.concatenate([mid_detail[(ex * 9 + e) * 8 : (ex * 9 + e) * 8 + 8] for e in range(9)], axis=1)
        for ex in range(3)
    ]
    low_lane = lax.broadcasted_iota(jnp.int32, (8, 128), 1) < 64
    coarse_blocks = []
    for ex in range(3):
        got = []
        for e in range(9):
            named = loaded["coarse_nbr"][my_parent, ex * 9 + e]
            got.append(jnp.where(named >= 0, coarse_tab[jnp.maximum(named, 0)], 0.0))
        pairs = [jnp.where(low_lane, got[e], got[e + 1]) for e in range(0, 8, 2)] + [got[8][:, :64]]
        coarse_blocks.append(jnp.concatenate(pairs, axis=1))

    def apply_one(level, blocks):
        parts = []
        if level > 0:
            parts.append(jnp.zeros((24 * level, 576), F32))
        parts += blocks
        if level < levels - 1:
            parts.append(jnp.zeros((24 * (levels - 1 - level), 576), F32))
        mixed = dot(mixers[...], jnp.concatenate(parts, axis=0).astype(BF16)).astype(BF16)
        total = None
        for at in range(0, terms // QUAD):
            got = dot(mixed[at * 32 : at * 32 + 32], tables[level, :, at * 256 : at * 256 + 256])
            total = got if total is None else total + got
        result = total[:8, :64]
        for k in range(1, QUAD):
            result = result + total[8 * k : 8 * k + 8, 64 * k : 64 * k + 64]
        return result

    coarse_out = apply_one(2, coarse_blocks)
    mid_direct = apply_one(1, mid_blocks)
    plane = open_plane(coarse_out)
    my_jl = my_octant & 3
    mine = plane[:, :64]
    for jl in range(1, 4):
        mine = jnp.where(my_jl == jl, plane[:, 64 * jl : 64 * jl + 64], mine)
    own_out = jnp.where(my_octant >= 4, held["own_out"][1], held["own_out"][0]).astype(BF16)
    mid_out = mid_direct + dot(own_out, triple(mine))
    for a in range(8):
        mid_ref[0:1, 64 * a : 64 * a + 64] = mid_out[a : a + 1]

    for cell in others:
        @pl.when(inside(steps[cell]))
        def _(cell=cell):
            halo_copy(26 - cell).wait_recv()
    wanted = halo[...].astype(F32).reshape(216, 512).astype(BF16)
    got = dot(picks[...], wanted)
    blocks = []
    for ex in range(3):
        for a in range(8):
            blocks.append(jnp.concatenate(
                [got[(ex * 9 + e) * 8 : (ex * 9 + e) * 8 + 8, 64 * a : 64 * a + 64] for e in range(9)], axis=1))
    sources = jnp.concatenate(blocks, axis=0).astype(BF16)
    total = None
    for at in range(terms // QUAD):
        spread = dot(sources, tables[0, :, at * 256 : at * 256 + 256]).astype(BF16)
        part = dot(block_mix[at * 256 : at * 256 + 256, :], spread)
        total = part if total is None else total + part
    direct = total[:64, :64]
    for k in range(1, QUAD):
        direct = direct + total[64 * k : 64 * k + 64, 64 * k : 64 * k + 64]
    fine = live * (direct + to_children(open_plane(mid_out)))
    fine_ref[...] = jnp.concatenate([fine[8 * x : 8 * x + 8] for x in range(8)], axis=1)

    pltpu.make_async_copy(all_rows, all_rows, row_send.at[0]).wait()
    for cell in others:
        @pl.when(inside(steps[cell]))
        def _(cell=cell):
            halo_copy(cell).wait_send()


SCALARS = ("mid_child", "mid_parent", "mid_refined", "mid_nbr", "coarse_nbr")


def shards(sizes, fine_coef, mid_leaf, mid_child, mid_parent, mid_refined, fine_nbr, mid_nbr, coarse_nbr,
           op_factor, term_weight):
    levels, terms = op_factor.shape[:2]
    coarse = coarse_nbr.shape[0]
    devices = math.prod(sizes)
    batch = math.gcd(coarse, 4)
    assert mid_child.shape == (1, 8) and fine_coef.shape == (8, 512) and terms % QUAD == 0
    args = dict(
        mid_child=mid_child, mid_parent=mid_parent, mid_refined=mid_refined, fine_coef=fine_coef,
        mid_leaf=mid_leaf, fine_nbr=fine_nbr, mid_nbr=mid_nbr, coarse_nbr=coarse_nbr,
        op_factor=jnp.transpose(op_factor, (0, 2, 3, 4, 1)), term_weight=term_weight[None, :],
    )
    consts = {name: jnp.asarray(value) for name, value in constants(terms, devices, batch).items()}
    arg_names, const_names = list(args), list(consts)
    dma = pltpu.SemaphoreType.DMA
    width = 64 * terms

    def buffer(name, value):
        space = pltpu.SMEM if name in SCALARS else pltpu.VMEM
        return space(value.shape, value.dtype)

    scratch = [buffer(name, value) for name, value in args.items()]
    scratch += [buffer(name, value) for name, value in consts.items()]
    scratch += [
        pltpu.VMEM((27, 8, 512), BF16),
        pltpu.VMEM((devices, 8, 128), BF16),
        pltpu.VMEM((levels * 3, 8, width), F32),
        pltpu.VMEM((levels * 3, 8, width), F32),
        pltpu.VMEM((levels, 576, width), BF16),
        pltpu.VMEM((8 * terms, 24 * levels), BF16),
        pltpu.VMEM((8 * terms, 192), F32),
        pltpu.VMEM((64 * terms, 192), BF16),
        pltpu.VMEM((216, 216), BF16),
        pltpu.VMEM((coarse, 8, 128), F32),
        dma((len(args),)), dma((len(consts),)), dma((1,)), dma((1,)), dma((27,)), dma((27,)),
    ]

    def body(*refs):
        n_args, n_consts = len(arg_names), len(const_names)
        ins, refs = refs[: n_args + n_consts], refs[n_args + n_consts :]
        outs, refs = refs[:2], refs[2:]
        loaded = dict(zip(arg_names, refs[:n_args]))
        held = dict(zip(const_names, refs[n_args : n_args + n_consts]))
        kernel(sizes, None, batch, levels, terms, coarse, dict(zip(arg_names, ins[:n_args])),
               dict(zip(const_names, ins[n_args:])), outs, (loaded, held) + tuple(refs[n_args + n_consts :]))

    vmem = pl.BlockSpec(memory_space=pltpu.VMEM)
    hbm = pl.BlockSpec(memory_space=pl.ANY)
    return pl.pallas_call(
        body,
        out_shape=(jax.ShapeDtypeStruct((8, 512), F32), jax.ShapeDtypeStruct((1, 512), F32)),
        in_specs=[hbm] * (len(args) + len(consts)),
        out_specs=(vmem, vmem),
        scratch_shapes=scratch,
        compiler_params=pltpu.CompilerParams(
            collective_id=0, has_side_effects=True, vmem_limit_bytes=58 * 1024 * 1024),
        name="tree",
    )(*args.values(), *consts.values())


def solution(mesh):
    sizes = tuple(mesh.shape[axis] for axis in AXES)
    split = P(AXES, None)
    line = P(AXES)
    return jax.shard_map(
        lambda *args: shards(sizes, *args),
        mesh=mesh,
        in_specs=(split, split, split, line, line, split, split, P(), P(), P()),
        out_specs=(split, split),
        check_vma=False,
    )
```

```python
import math

import jax
import jax.numpy as jnp
import numpy as np
from jax import lax
from jax.experimental import pallas as pl
from jax.experimental.pallas import tpu as pltpu
from jax.sharding import PartitionSpec as P

MESH = pl.DeviceIdType.MESH
AXES = ("gx", "gy", "gz")
CENTRE = 13
QUAD = 4
F32 = jnp.float32
BF16 = jnp.bfloat16


def poly_multiply(left, right):
    result = [0.0] * (len(left) + len(right) - 1)
    for first, left_coef in enumerate(left):
        for second, right_coef in enumerate(right):
            result[first + second] += left_coef * right_coef
    return result


def poly_compose(coeffs, factor, offset):
    result = [0.0]
    power_term = [1.0]
    for coef in coeffs:
        padded = result + [0.0] * (len(power_term) - len(result))
        result = [padded[place] + coef * power_term[place] for place in range(len(power_term))]
        power_term = poly_multiply(power_term, [offset, factor])
    return result


def legendre_table(basis_order):
    polys = [[1.0], [0.0, 1.0]]
    for degree in range(1, basis_order):
        upper = [0.0] + [(2 * degree + 1) * coef for coef in polys[degree]]
        lower = [degree * coef for coef in polys[degree - 1]] + [0.0] * (
            len(upper) - len(polys[degree - 1])
        )
        polys.append([(upper[place] - lower[place]) / (degree + 1) for place in range(len(upper))])
    return [
        [math.sqrt(2 * degree + 1) * coef for coef in poly_compose(polys[degree], 2.0, -1.0)]
        for degree in range(basis_order)
    ]


def two_scale(basis_order):
    shifted = legendre_table(basis_order)
    filters = np.zeros((2, basis_order, basis_order))
    for which_half in range(2):
        for row_at in range(basis_order):
            halved = poly_compose(shifted[row_at], 0.5, 0.5 * which_half)
            for col_at in range(basis_order):
                product = poly_multiply(halved, shifted[col_at])
                total = sum((coef / (place + 1) for place, coef in enumerate(product)))
                filters[which_half, row_at, col_at] = total / math.sqrt(2.0)
    return np.asarray(filters, np.float32)


def halves(array):
    high = array.astype(BF16)
    return high, (array - high.astype(array.dtype)).astype(BF16)


def np_halves(array):
    array = np.asarray(array, np.float32)
    high = array.astype(BF16)
    return high, (array - high.astype(np.float32)).astype(BF16)


def dot(left, right):
    return jnp.dot(left, right, preferred_element_type=F32)


def dot_rows(left, right):
    return lax.dot_general(left, right, (((1,), (1,)), ((), ())), preferred_element_type=F32)


def constants(terms, devices, batch):
    filters = two_scale(8)
    table = {}
    row = np.arange(8 * terms)
    lane = np.arange(64 * terms)
    same = (row % terms)[:, None] == (lane // 64)[None, :]
    spread = [same & ((row // terms)[:, None] == part[None, :]) for part in (lane // 8 % 8, lane % 8)]
    table["spread"] = np.concatenate(spread, axis=1).astype(BF16)
    swap = (row // 8)[:, None] == (row % terms)[None, :]
    swap &= (row % 8)[:, None] == (row // terms)[None, :]
    table["swap"] = swap.astype(BF16)
    table["widen"] = (np.arange(72)[:, None] == (np.arange(192) // 8)[None, :]).astype(BF16)
    plane = np.einsum("jqy,lrz->jlyzqr", filters, filters)
    table["gather_plane"] = np.concatenate(np_halves(plane.reshape(256, 64)), axis=1)
    plane = np.einsum("jqy,lrz->qrjlyz", filters, filters)
    table["scatter_plane"] = np.concatenate(np_halves(plane.reshape(64, 256)), axis=1)
    parts = [np.asarray(part, np.float32) for part in np_halves(filters)]
    both = np.stack(parts, axis=1).reshape(4, 8, 8)
    flip = np.swapaxes(both, 1, 2)
    table["child_in"] = np.repeat(both, 8, axis=2)
    table["child_out"] = np.tile(np.repeat(flip, 8, axis=1), (1, 1, 4))
    table["mid_in"] = np.tile(both, (1, 1, devices))
    table["mid_out"] = np.tile(flip, (1, 1, batch * 4))
    own = [np.concatenate([flip[2 * i], flip[2 * i], flip[2 * i + 1]], axis=1) for i in range(2)]
    table["own_out"] = np.stack(own)
    cell = np.arange(27 * 8) // 8
    cells = np.zeros((8, 27 * 8), np.int32)
    cells[:4] = np.stack([cell // 9 - 1, cell // 3 % 3 - 1, cell % 3 - 1, np.arange(27 * 8) % 8])
    table["cells"] = cells
    return table


def kernel(sizes, names, batch, levels, terms, coarse, args, consts, outs, scratch):
    size_x, size_y, size_z = sizes
    devices = size_x * size_y * size_z
    here = [lax.axis_index(axis) for axis in AXES]
    me = (here[0] * size_y + here[1]) * size_z + here[2]
    fine_ref, mid_ref = outs
    (loaded, held, halo, rows, factor_left, factor_right, tables, mixers, mixers_t, block_mix, picks, coarse_tab,
     load_sem, held_sem, row_send, row_recv, halo_send, halo_recv) = scratch

    def each_peer(body):
        if devices <= 64:
            spots = [
                [at] + [lax.rem(at + k, size) for k in range(1, size)] for at, size in zip(here, sizes)
            ]
            peers = [(x, y, z) for x in spots[0] for y in spots[1] for z in spots[2]]
            for peer in peers[1:]:
                body(peer)
        else:
            def step(offset, carry):
                device = lax.rem(me + offset, devices)
                body((device // (size_y * size_z), device // size_z % size_y, device % size_z))
                return carry
            lax.fori_loop(1, devices, step, 0)

    loads = {}
    for at, (name, source) in enumerate(args.items()):
        loads[name] = pltpu.make_async_copy(source, loaded[name], load_sem.at[at])
    for at, (name, source) in enumerate(consts.items()):
        loads[name] = pltpu.make_async_copy(source, held[name], held_sem.at[at])
    order = ["mid_child", "mid_parent", "mid_refined", "fine_coef", "mid_leaf", "child_in", "gather_plane",
             "child_out", "scatter_plane"]
    order += [name for name in loads if name not in order]
    for name in order:
        loads[name].start()

    barrier = pltpu.get_barrier_semaphore()
    each_peer(lambda peer: pl.semaphore_signal(
        barrier, inc=1, device_id=peer, device_id_type=MESH))

    def ready(*wanted):
        for name in wanted:
            loads[name].wait()

    ready("mid_child", "mid_parent", "mid_refined", "fine_coef", "mid_leaf", "child_in", "gather_plane")
    child = [loaded["mid_child"][0, o] for o in range(8)]
    refined = loaded["mid_refined"][0] > 0
    live = jnp.where(refined, 1.0, 0.0).astype(F32)
    mid_parent = loaded["mid_parent"][0]
    my_parent = lax.shift_right_logical(mid_parent, 3)
    my_octant = mid_parent & 7
    flat = loaded["fine_coef"][...].astype(F32)
    by_row = jnp.concatenate([flat[:, 64 * x : 64 * x + 64] for x in range(8)], axis=0)
    slot_lane = lax.broadcasted_iota(jnp.int32, (8, 64), 1) & 7
    child_in = [held["child_in"][k] for k in range(4)]
    blocks = []
    for part in range(2):
        for jl in range(4):
            block = jnp.where(slot_lane == child[jl], child_in[part], 0.0)
            blocks.append(block + jnp.where(slot_lane == child[4 + jl], child_in[2 + part], 0.0))
    mixed = dot(jnp.concatenate(blocks, axis=0).astype(BF16), by_row.astype(BF16))
    mixed = mixed[:32] + mixed[32:]

    def stack_halves(array):
        high, low = halves(array)
        return jnp.concatenate([high.astype(F32), low.astype(F32)], axis=0).astype(BF16)

    def close_children(mixed, boxes):
        wide = [
            jnp.concatenate([mixed[(4 * k + jl) * 8 : (4 * k + jl) * 8 + 8] for jl in range(4)], axis=1)
            for k in range(boxes)
        ]
        wide = wide[0] if boxes == 1 else jnp.concatenate(wide, axis=0)
        got = dot(stack_halves(wide), held["gather_plane"][...])
        count = boxes * 8
        return got[:count, :64] + got[:count, 64:] + got[count:, :64]

    def open_plane(block, exact=False):
        count = block.shape[0]
        if exact:
            got = dot(block.astype(BF16), held["scatter_plane"][...])
            return got[:, :256] + got[:, 256:]
        got = dot(stack_halves(block), held["scatter_plane"][...])
        return got[:count, :256] + got[:count, 256:] + got[count:, :256]

    def lanes_to_rows(plane):
        count = plane.shape[0] // 8
        return jnp.concatenate(
            [plane[8 * k : 8 * k + 8, 64 * jl : 64 * jl + 64] for k in range(count) for jl in range(4)], axis=0
        )

    def triple(rows_f32):
        high, low = halves(rows_f32)
        high, low = high.astype(F32), low.astype(F32)
        return jnp.concatenate([high, low, high], axis=0).astype(BF16)

    compressed = close_children(mixed, 1)
    leaf = jnp.broadcast_to(loaded["mid_leaf"][...].astype(F32), (8, 512))
    block_lane = lax.shift_right_logical(lax.broadcasted_iota(jnp.int32, (8, 512), 1), 6)
    leaf = jnp.where(block_lane == lax.broadcasted_iota(jnp.int32, (8, 512), 0), leaf, 0.0)
    leaf_square = leaf[:, :64]
    for x in range(1, 8):
        leaf_square = leaf_square + leaf[:, 64 * x : 64 * x + 64]
    mid_source = jnp.where(refined, compressed, leaf_square).astype(BF16).astype(F32)
    note = lax.broadcasted_iota(jnp.int32, (8, 64), 1)
    place = jnp.where(note == 0, my_parent + 1, jnp.where(note == 1, my_octant, 0)).astype(F32)
    rows[me] = jnp.concatenate([mid_source, place], axis=1).astype(BF16)

    ready("child_out", "scatter_plane")
    jl_lane = lax.shift_right_logical(lax.broadcasted_iota(jnp.int32, (64, 32), 1), 3)
    slot_row = lax.broadcasted_iota(jnp.int32, (64, 32), 0) & 7

    def child_lane(i):
        return jnp.where(jl_lane == 0, child[4 * i],
                         jnp.where(jl_lane == 1, child[4 * i + 1],
                                   jnp.where(jl_lane == 2, child[4 * i + 2], child[4 * i + 3])))

    chosen = [slot_row == child_lane(i) for i in range(2)]
    out_parts = [
        jnp.where(chosen[0], held["child_out"][part], 0.0)
        + jnp.where(chosen[1], held["child_out"][2 + part], 0.0)
        for part in range(2)
    ]
    child_out = jnp.concatenate([out_parts[0], out_parts[0], out_parts[1]], axis=1).astype(BF16)

    def to_children(plane):
        return dot(child_out, triple(lanes_to_rows(plane)))

    detail = live * (by_row - to_children(open_plane(mid_source, exact=True)))
    detail = jnp.concatenate([detail[8 * x : 8 * x + 8] for x in range(8)], axis=1)
    halo[CENTRE] = detail.astype(BF16)

    steps = [(c // 9 - 1, c // 3 % 3 - 1, c % 3 - 1) for c in range(27)]

    def inside(step):
        tests = []
        for at, size, move in zip(here, sizes, step):
            if move == 1:
                tests.append(at < size - 1)
            elif move == -1:
                tests.append(at > 0)
        found = tests[0]
        for test in tests[1:]:
            found = found & test
        return found

    def halo_copy(cell):
        move = steps[cell]
        peer = tuple(at + part for at, part in zip(here, move))
        return pltpu.make_async_remote_copy(
            src_ref=halo.at[CENTRE],
            dst_ref=halo.at[26 - cell],
            send_sem=halo_send.at[cell],
            recv_sem=halo_recv.at[26 - cell],
            device_id=peer,
            device_id_type=MESH,
        )

    others = [cell for cell in range(27) if cell != CENTRE]
    pl.semaphore_wait(barrier, devices - 1)
    each_peer(lambda peer: pltpu.make_async_remote_copy(
        src_ref=rows.at[me],
        dst_ref=rows.at[me],
        send_sem=row_send.at[0],
        recv_sem=row_recv.at[0],
        device_id=peer,
        device_id_type=MESH,
    ).start())

    for cell in others:
        @pl.when(inside(steps[cell]))
        def _(cell=cell):
            halo_copy(cell).start()

        @pl.when(jnp.logical_not(inside(steps[cell])))
        def _(cell=cell):
            halo[cell] = jnp.zeros(halo.shape[1:], BF16)

    ready("op_factor", "term_weight", "spread", "swap", "widen")
    factor = loaded["op_factor"]
    planes = []
    for level in range(levels):
        for e in range(3):
            planes.append(jnp.concatenate([factor[level, e, b] for b in range(8)], axis=1))
    plane = jnp.concatenate(planes, axis=0)
    weight = jnp.concatenate([loaded["term_weight"][...]] * 8, axis=1)
    rounded = plane.astype(BF16)
    left_side = stack_halves(plane * weight)
    right_side = stack_halves(plane)
    count = plane.shape[0]
    width = 64 * terms
    for at in range(0, width, 512):
        got = dot(left_side, held["spread"][:, at : at + 512])
        got = got[:count] + got[count:]
        factor_left[:, :, at : at + 512] = got.reshape(levels * 3, 8, 512)
        got = dot(right_side, held["spread"][:, width + at : width + at + 512])
        got = got[:count] + got[count:]
        factor_right[:, :, at : at + 512] = got.reshape(levels * 3, 8, 512)
    turned = dot_rows(held["swap"][...], rounded).astype(BF16)
    mixers[...] = turned
    mixers_t[...] = dot(turned, held["widen"][...])

    def table_step(at, carry):
        level, ey = at // 3, at % 3
        left = factor_left.at[at]
        for ez in range(3):
            right = factor_right[level * 3 + ez]
            base = (ey * 3 + ez) * 64
            for k in range(4):
                pair = [left[2 * k + half : 2 * k + half + 1, :] * right for half in range(2)]
                start = pl.multiple_of(base + 16 * k, 16)
                tables[level, pl.ds(start, 16), :] = jnp.concatenate(pair, axis=0).astype(BF16)
        return carry

    lax.fori_loop(0, levels * 3, table_step, 0)
    own_lane = (lax.broadcasted_iota(jnp.int32, (8, 192), 1) & 7) == lax.broadcasted_iota(jnp.int32, (8, 192), 0)

    def mix_step(at, carry):
        some = mixers_t[pl.ds(pl.multiple_of(at * 16, 16), 16), :]
        some = jnp.where(own_lane[None], jnp.broadcast_to(some[:, None, :], (16, 8, 192)), 0.0)
        block_mix[pl.ds(pl.multiple_of(at * 128, 128), 128), :] = some.reshape(128, 192).astype(BF16)
        return carry

    lax.fori_loop(0, terms // 2, mix_step, 0)

    ready("cells", "fine_nbr")
    cells = held["cells"]
    spot = [here[k] + cells[k : k + 1, :] for k in range(3)]
    there = None
    for k in range(3):
        test = (spot[k] >= 0) & (spot[k] < sizes[k])
        there = test if there is None else there & test
    names_row = ((spot[0] * size_y + spot[1]) * size_z + spot[2]) * 8 + cells[3:4, :]
    names_row = jnp.where(there, names_row, -2)
    near = loaded["fine_nbr"][...]
    hot = [(near[:, d : d + 1] == names_row).astype(F32) for d in range(27)]
    picks[...] = jnp.concatenate(hot, axis=0).astype(BF16)

    for cell in others:
        @pl.when(inside(steps[cell]))
        def _(cell=cell):
            halo_copy(26 - cell).wait_recv()

    wanted = halo[...].astype(F32).reshape(216, 512).astype(BF16)
    got = dot(picks[...], wanted)
    blocks = []
    for ex in range(3):
        for a in range(8):
            blocks.append(jnp.concatenate(
                [got[(ex * 9 + e) * 8 : (ex * 9 + e) * 8 + 8, 64 * a : 64 * a + 64] for e in range(9)], axis=1))
    sources = jnp.concatenate(blocks, axis=0).astype(BF16)
    total = None
    for at in range(terms // QUAD):
        spread = dot(sources, tables[0, :, at * 256 : at * 256 + 256]).astype(BF16)
        part = dot(block_mix[at * 256 : at * 256 + 256, :], spread)
        total = part if total is None else total + part
    direct = total[:64, :64]
    for k in range(1, QUAD):
        direct = direct + total[64 * k : 64 * k + 64, 64 * k : 64 * k + 64]

    ready("mid_in", "mid_out", "own_out", "mid_nbr", "coarse_nbr")
    all_rows = rows.at[pl.ds(0, devices - 1)]
    pltpu.make_async_copy(all_rows, all_rows, row_recv.at[0]).wait()
    gathered = rows[...].astype(F32).reshape(devices * 8, 128).astype(BF16)
    reader_lane = lax.broadcasted_iota(jnp.int32, (8, 128), 1)
    reader = jnp.where(reader_lane == 64, 8.0, jnp.where(reader_lane == 65, 1.0, 0.0)).astype(BF16)
    code = dot_rows(reader, gathered) - 8.0
    near_rows = []
    for d in range(27):
        named = loaded["mid_nbr"][0, d]
        got = rows[jnp.maximum(named, 0)].astype(F32)
        near_rows.append(jnp.where(named >= 0, got, 0.0))
    near_rows = jnp.concatenate(near_rows, axis=0)
    near_code = near_rows[:, 64:65] * 8.0 + near_rows[:, 65:66] - 8.0
    batch_lane = lax.broadcasted_iota(jnp.int32, (8, batch * 32), 1)
    batch_code = lax.shift_right_logical(batch_lane, 5) * 8 + (lax.shift_right_logical(batch_lane, 3) & 3)

    def coarse_step(at, total):
        first = at * (batch * 8)
        first_f = first.astype(F32) if hasattr(first, "astype") else float(first)
        blocks = []
        for part in range(2):
            for k in range(batch):
                for jl in range(4):
                    want = first_f + float(8 * k + jl)
                    block = jnp.where(code == want, held["mid_in"][part], 0.0)
                    blocks.append(block + jnp.where(code == want + 4.0, held["mid_in"][2 + part], 0.0))
        mixed = dot(jnp.concatenate(blocks, axis=0).astype(BF16), gathered)
        half = batch * 32
        source = close_children(mixed[:half, :64] + mixed[half:, :64], batch)
        held_source = source.astype(BF16).astype(F32)
        double = jnp.concatenate([held_source, held_source], axis=1)
        coarse_tab[pl.ds(at * batch, batch)] = double.reshape(batch, 8, 128)
        lane_code = first_f + batch_code.astype(F32)
        parts = [[], []]
        for d in range(27):
            mine = near_code[8 * d : 8 * d + 8]
            lower, upper = mine == lane_code, mine == lane_code + 4.0
            for part in range(2):
                block = jnp.where(lower, held["mid_out"][part], 0.0)
                parts[part].append(block + jnp.where(upper, held["mid_out"][2 + part], 0.0))
        parts = [jnp.concatenate(part, axis=0).astype(BF16) for part in parts]
        spread = triple(lanes_to_rows(open_plane(source)))
        rows_out = dot(jnp.concatenate([parts[0], parts[0], parts[1]], axis=1), spread)
        return total + rows_out

    batches = coarse // batch
    zero = jnp.zeros((216, 64), F32)
    from_coarse = coarse_step(0, zero) if batches == 1 else lax.fori_loop(0, batches, coarse_step, zero)
    mid_detail = near_rows[:, :64] - from_coarse
    mid_blocks = [
        jnp.concatenate([mid_detail[(ex * 9 + e) * 8 : (ex * 9 + e) * 8 + 8] for e in range(9)], axis=1)
        for ex in range(3)
    ]
    low_lane = lax.broadcasted_iota(jnp.int32, (8, 128), 1) < 64
    coarse_blocks = []
    for ex in range(3):
        got = []
        for e in range(9):
            named = loaded["coarse_nbr"][my_parent, ex * 9 + e]
            got.append(jnp.where(named >= 0, coarse_tab[jnp.maximum(named, 0)], 0.0))
        pairs = [jnp.where(low_lane, got[e], got[e + 1]) for e in range(0, 8, 2)] + [got[8][:, :64]]
        coarse_blocks.append(jnp.concatenate(pairs, axis=1))

    def apply_one(level, blocks):
        parts = []
        if level > 0:
            parts.append(jnp.zeros((24 * level, 576), F32))
        parts += blocks
        if level < levels - 1:
            parts.append(jnp.zeros((24 * (levels - 1 - level), 576), F32))
        mixed = dot(mixers[...], jnp.concatenate(parts, axis=0).astype(BF16)).astype(BF16)
        total = None
        for at in range(0, terms // QUAD):
            got = dot(mixed[at * 32 : at * 32 + 32], tables[level, :, at * 256 : at * 256 + 256])
            total = got if total is None else total + got
        result = total[:8, :64]
        for k in range(1, QUAD):
            result = result + total[8 * k : 8 * k + 8, 64 * k : 64 * k + 64]
        return result

    coarse_out = apply_one(2, coarse_blocks)
    mid_direct = apply_one(1, mid_blocks)
    plane = open_plane(coarse_out)
    my_jl = my_octant & 3
    mine = plane[:, :64]
    for jl in range(1, 4):
        mine = jnp.where(my_jl == jl, plane[:, 64 * jl : 64 * jl + 64], mine)
    own_out = jnp.where(my_octant >= 4, held["own_out"][1], held["own_out"][0]).astype(BF16)
    mid_out = mid_direct + dot(own_out, triple(mine))
    for a in range(8):
        mid_ref[0:1, 64 * a : 64 * a + 64] = mid_out[a : a + 1]

    fine = live * (direct + to_children(open_plane(mid_out)))
    fine_ref[...] = jnp.concatenate([fine[8 * x : 8 * x + 8] for x in range(8)], axis=1)

    pltpu.make_async_copy(all_rows, all_rows, row_send.at[0]).wait()
    for cell in others:
        @pl.when(inside(steps[cell]))
        def _(cell=cell):
            halo_copy(cell).wait_send()


SCALARS = ("mid_child", "mid_parent", "mid_refined", "mid_nbr", "coarse_nbr")


def shards(sizes, fine_coef, mid_leaf, mid_child, mid_parent, mid_refined, fine_nbr, mid_nbr, coarse_nbr,
           op_factor, term_weight):
    levels, terms = op_factor.shape[:2]
    coarse = coarse_nbr.shape[0]
    devices = math.prod(sizes)
    batch = math.gcd(coarse, 4)
    assert mid_child.shape == (1, 8) and fine_coef.shape == (8, 512) and terms % QUAD == 0
    args = dict(
        mid_child=mid_child, mid_parent=mid_parent, mid_refined=mid_refined, fine_coef=fine_coef,
        mid_leaf=mid_leaf, fine_nbr=fine_nbr, mid_nbr=mid_nbr, coarse_nbr=coarse_nbr,
        op_factor=jnp.transpose(op_factor, (0, 2, 3, 4, 1)), term_weight=term_weight[None, :],
    )
    consts = {name: jnp.asarray(value) for name, value in constants(terms, devices, batch).items()}
    arg_names, const_names = list(args), list(consts)
    dma = pltpu.SemaphoreType.DMA
    width = 64 * terms

    def buffer(name, value):
        space = pltpu.SMEM if name in SCALARS else pltpu.VMEM
        return space(value.shape, value.dtype)

    scratch = [buffer(name, value) for name, value in args.items()]
    scratch += [buffer(name, value) for name, value in consts.items()]
    scratch += [
        pltpu.VMEM((27, 8, 512), BF16),
        pltpu.VMEM((devices, 8, 128), BF16),
        pltpu.VMEM((levels * 3, 8, width), F32),
        pltpu.VMEM((levels * 3, 8, width), F32),
        pltpu.VMEM((levels, 576, width), BF16),
        pltpu.VMEM((8 * terms, 24 * levels), BF16),
        pltpu.VMEM((8 * terms, 192), F32),
        pltpu.VMEM((64 * terms, 192), BF16),
        pltpu.VMEM((216, 216), BF16),
        pltpu.VMEM((coarse, 8, 128), F32),
        dma((len(args),)), dma((len(consts),)), dma((1,)), dma((1,)), dma((27,)), dma((27,)),
    ]

    def body(*refs):
        n_args, n_consts = len(arg_names), len(const_names)
        ins, refs = refs[: n_args + n_consts], refs[n_args + n_consts :]
        outs, refs = refs[:2], refs[2:]
        loaded = dict(zip(arg_names, refs[:n_args]))
        held = dict(zip(const_names, refs[n_args : n_args + n_consts]))
        kernel(sizes, None, batch, levels, terms, coarse, dict(zip(arg_names, ins[:n_args])),
               dict(zip(const_names, ins[n_args:])), outs, (loaded, held) + tuple(refs[n_args + n_consts :]))

    vmem = pl.BlockSpec(memory_space=pltpu.VMEM)
    hbm = pl.BlockSpec(memory_space=pltpu.HBM)
    shapes = ((8, 512), (1, 512))
    inner = pl.pallas_call(
        body,
        out_shape=tuple(pltpu.VMEM(shape, F32) for shape in shapes),
        in_specs=[hbm] * (len(args) + len(consts)),
        out_specs=(vmem, vmem),
        scratch_shapes=scratch,
        compiler_params=pltpu.CompilerParams(
            collective_id=0, has_side_effects=True, vmem_limit_bytes=58 * 1024 * 1024),
        name="tree",
    )(*args.values(), *consts.values())

    def store(fine_in, mid_in, fine_to, mid_to, sem):
        copies = [
            pltpu.make_async_copy(fine_in, fine_to, sem.at[0]),
            pltpu.make_async_copy(mid_in, mid_to, sem.at[1]),
        ]
        for copy in copies:
            copy.start()
        for copy in copies:
            copy.wait()

    return pl.pallas_call(
        store,
        out_shape=tuple(jax.ShapeDtypeStruct(shape, F32) for shape in shapes),
        in_specs=[pl.BlockSpec(memory_space=pl.ANY)] * 2,
        out_specs=(hbm, hbm),
        scratch_shapes=[dma((2,))],
        compiler_params=pltpu.CompilerParams(vmem_limit_bytes=1 << 20),
        name="store",
    )(*inner)


def solution(mesh):
    sizes = tuple(mesh.shape[axis] for axis in AXES)
    split = P(AXES, None)
    line = P(AXES)
    return jax.shard_map(
        lambda *args: shards(sizes, *args),
        mesh=mesh,
        in_specs=(split, split, split, line, line, split, split, P(), P(), P()),
        out_specs=(split, split),
        check_vma=False,
    )
```

```python
import math

import jax
import jax.numpy as jnp
import numpy as np
from jax import lax
from jax.experimental import pallas as pl
from jax.experimental.pallas import tpu as pltpu
from jax.sharding import PartitionSpec as P

MESH = pl.DeviceIdType.MESH
AXES = ("gx", "gy", "gz")
CENTRE = 13
QUAD = 4
EARLY = 1
GROUPS = 4
F32 = jnp.float32
BF16 = jnp.bfloat16


def poly_multiply(left, right):
    result = [0.0] * (len(left) + len(right) - 1)
    for first, left_coef in enumerate(left):
        for second, right_coef in enumerate(right):
            result[first + second] += left_coef * right_coef
    return result


def poly_compose(coeffs, factor, offset):
    result = [0.0]
    power_term = [1.0]
    for coef in coeffs:
        padded = result + [0.0] * (len(power_term) - len(result))
        result = [padded[place] + coef * power_term[place] for place in range(len(power_term))]
        power_term = poly_multiply(power_term, [offset, factor])
    return result


def legendre_table(basis_order):
    polys = [[1.0], [0.0, 1.0]]
    for degree in range(1, basis_order):
        upper = [0.0] + [(2 * degree + 1) * coef for coef in polys[degree]]
        lower = [degree * coef for coef in polys[degree - 1]] + [0.0] * (
            len(upper) - len(polys[degree - 1])
        )
        polys.append([(upper[place] - lower[place]) / (degree + 1) for place in range(len(upper))])
    return [
        [math.sqrt(2 * degree + 1) * coef for coef in poly_compose(polys[degree], 2.0, -1.0)]
        for degree in range(basis_order)
    ]


def two_scale(basis_order):
    shifted = legendre_table(basis_order)
    filters = np.zeros((2, basis_order, basis_order))
    for which_half in range(2):
        for row_at in range(basis_order):
            halved = poly_compose(shifted[row_at], 0.5, 0.5 * which_half)
            for col_at in range(basis_order):
                product = poly_multiply(halved, shifted[col_at])
                total = sum((coef / (place + 1) for place, coef in enumerate(product)))
                filters[which_half, row_at, col_at] = total / math.sqrt(2.0)
    return np.asarray(filters, np.float32)


def halves(array):
    high = array.astype(BF16)
    return high, (array - high.astype(array.dtype)).astype(BF16)


def np_halves(array):
    array = np.asarray(array, np.float32)
    high = array.astype(BF16)
    return high, (array - high.astype(np.float32)).astype(BF16)


def dot(left, right):
    return jnp.dot(left, right, preferred_element_type=F32)


def dot_rows(left, right):
    return lax.dot_general(left, right, (((1,), (1,)), ((), ())), preferred_element_type=F32)


def constants(terms, devices, batch):
    filters = two_scale(8)
    exact = np.asarray(filters, np.float64)
    table = {}
    row = np.arange(8 * terms)
    lane = np.arange(64 * QUAD)
    same = (row % terms)[:, None] == (lane // 64)[None, :]
    spread = [same & ((row // terms)[:, None] == part[None, :]) for part in (lane // 8 % 8, lane % 8)]
    table["spread"] = np.concatenate(spread, axis=1).astype(BF16)
    swap = (row // 8)[:, None] == (row % terms)[None, :]
    swap &= (row % 8)[:, None] == (row // terms)[None, :]
    table["swap"] = swap.astype(BF16)
    table["widen"] = (np.arange(72)[:, None] == (np.arange(192) // 8)[None, :]).astype(BF16)
    close = np.einsum("jqy,lrz->jlyzqr", exact, exact).reshape(256, 64)
    opened = np.ascontiguousarray(close.T)
    twice = np.concatenate([close, close], axis=1)
    table["close"] = np.concatenate(np_halves(twice), axis=1)
    table["open"] = np.concatenate([np.concatenate(np_halves(opened), axis=1)] * 2, axis=0)
    table["coarse"] = np.concatenate(np_halves(twice) + np_halves(close @ opened), axis=1)
    fold = np.tile(np.eye(64, dtype=np.float32), (2, 2)).astype(BF16)
    stack = np.tile(opened, (2, 1))
    table["mid_tail"] = np.concatenate((fold,) + np_halves(stack), axis=1)
    tails = []
    for jl in range(4):
        mine = opened[:, 64 * jl : 64 * jl + 64]
        both = np.tile(np.concatenate([mine, mine], axis=1), (2, 1))
        tails.append(np.concatenate(np_halves(both) + np_halves(np.tile(mine @ opened, (2, 1))), axis=1))
    table["coarse_tail"] = np.stack(tails)
    parts = [np.asarray(part, np.float32) for part in np_halves(filters)]
    both = np.stack(parts, axis=1).reshape(4, 8, 8)
    flip = np.swapaxes(both, 1, 2)
    table["child_in"] = np.repeat(both, 8, axis=2)
    chains = [[exact[i].T for i in range(2)]]
    chains += [[exact[i].T @ exact[own].T for i in range(2)] for own in range(2)]
    out = np.stack([np.stack(np_halves(chain)) for chain_set in chains for chain in chain_set])
    out = np.asarray(out, np.float32).reshape(12, 8, 8)
    table["child_out"] = np.tile(np.repeat(out, 8, axis=1), (1, 1, 2))
    table["mid_in"] = np.tile(both, (1, 1, devices))
    table["mid_out"] = np.tile(flip, (1, 1, batch))
    own = [np.concatenate([flip[2 * i], flip[2 * i], flip[2 * i + 1]], axis=1) for i in range(2)]
    table["own_out"] = np.stack(own)
    cell = np.arange(27 * 8) // 8
    cells = np.zeros((8, 27 * 8), np.int32)
    cells[:4] = np.stack([cell // 9 - 1, cell // 3 % 3 - 1, cell % 3 - 1, np.arange(27 * 8) % 8])
    table["cells"] = cells
    return table


def kernel(sizes, batch, levels, terms, coarse, args, consts, outs, scratch):
    size_x, size_y, size_z = sizes
    devices = size_x * size_y * size_z
    here = [lax.axis_index(axis) for axis in AXES]
    me = (here[0] * size_y + here[1]) * size_z + here[2]
    fine_ref, mid_ref = outs
    (loaded, held, halo, rows, codes, factor_left, factor_right, tables, mixers, mixers_t, block_mix, spreads, picks,
     coarse_tab, load_sem, held_sem, row_send, row_recv, code_send, code_recv, halo_send, halo_recv) = scratch

    def each_peer(body):
        if devices <= 64:
            spots = [
                [at] + [lax.rem(at + k, size) for k in range(1, size)] for at, size in zip(here, sizes)
            ]
            peers = [(x, y, z) for x in spots[0] for y in spots[1] for z in spots[2]]
            for peer in peers[1:]:
                body(peer)
        else:
            def step(offset, carry):
                device = lax.rem(me + offset, devices)
                body((device // (size_y * size_z), device // size_z % size_y, device % size_z))
                return carry
            lax.fori_loop(1, devices, step, 0)

    loads = {}
    for at, (name, source) in enumerate(args.items()):
        loads[name] = pltpu.make_async_copy(source, loaded[name], load_sem.at[at])
    for at, (name, source) in enumerate(consts.items()):
        loads[name] = pltpu.make_async_copy(source, held[name], held_sem.at[at])
    order = ["mid_child", "mid_parent", "mid_refined", "fine_coef", "mid_leaf", "child_in", "close",
             "child_out", "open"]
    order += [name for name in loads if name not in order]
    for name in order[:9]:
        loads[name].start()
    barrier = pltpu.get_barrier_semaphore()
    each_peer(lambda peer: pl.semaphore_signal(
        barrier, inc=1, device_id=peer, device_id_type=MESH))
    for name in order[9:]:
        loads[name].start()

    def ready(*wanted):
        for name in wanted:
            loads[name].wait()

    def turn(array):
        return pltpu.roll(array, 64, 1)

    def lanes(shape):
        return lax.broadcasted_iota(jnp.int32, shape, len(shape) - 1)

    def stack_halves(array):
        high, low = halves(array)
        return jnp.concatenate([high.astype(F32), low.astype(F32)], axis=0).astype(BF16)

    def triple(array):
        high, low = halves(array)
        high, low = high.astype(F32), low.astype(F32)
        return jnp.concatenate([high, low, high], axis=0)

    half_lane = lax.shift_right_logical(lanes((8, 128)), 6)
    low_lane = half_lane == 0

    ready("mid_child", "mid_parent", "mid_refined", "fine_coef", "mid_leaf", "child_in", "close")
    child = [loaded["mid_child"][0, o] for o in range(8)]
    refined = loaded["mid_refined"][0] > 0
    live = jnp.where(refined, 1.0, 0.0).astype(F32)
    mid_parent = loaded["mid_parent"][0]
    my_parent = lax.shift_right_logical(mid_parent, 3)
    my_octant = mid_parent & 7
    code_lane = lax.shift_right_logical(lanes((2, 128)), 3) == (me & 15)
    code_row = lax.broadcasted_iota(jnp.int32, (2, 128), 0) == 1
    codes[me] = jnp.where(code_lane | code_row, mid_parent + 1, 0).astype(F32)

    flat = loaded["fine_coef"][...].astype(F32)
    by_row = []
    for k in range(4):
        tile = flat[:, 128 * k : 128 * k + 128]
        turned = turn(tile)
        by_row += [jnp.where(low_lane, tile, turned), jnp.where(low_lane, turned, tile)]
    by_row = jnp.concatenate(by_row, axis=0)
    slot_lane = lanes((8, 64)) & 7
    child_in = [held["child_in"][k] for k in range(4)]
    blocks = []
    for part in range(2):
        for jl in range(4):
            block = jnp.where(slot_lane == child[jl], child_in[part], 0.0)
            blocks.append(block + jnp.where(slot_lane == child[4 + jl], child_in[2 + part], 0.0))
    mixed = dot(jnp.concatenate(blocks, axis=0).astype(BF16), by_row.astype(BF16))
    mixed = mixed[:32] + mixed[32:]
    wide = [jnp.where(low_lane, mixed[16 * j : 16 * j + 8], mixed[16 * j + 8 : 16 * j + 16]) for j in range(2)]
    got = dot(stack_halves(jnp.concatenate(wide, axis=1)), held["close"][...])
    compressed = got[:8, :128] + got[:8, 128:] + got[8:, :128]
    leaf = jnp.broadcast_to(loaded["mid_leaf"][...].astype(F32), (8, 512))
    leaf_block = lax.shift_right_logical(lanes((8, 512)), 6)
    leaf = jnp.where(leaf_block == lax.broadcasted_iota(jnp.int32, (8, 512), 0), leaf, 0.0)
    leaf = leaf[:, :128] + leaf[:, 128:256] + leaf[:, 256:384] + leaf[:, 384:]
    leaf = leaf + turn(leaf)
    mid_source = jnp.where(refined, compressed, leaf)
    placed = jnp.where(half_lane == (my_octant & 1), mid_source, 0.0).astype(BF16)
    rows[me] = placed

    ready("child_out", "open")
    j_lane = lax.shift_right_logical(lanes((64, 16)), 3)
    slot_row = lax.broadcasted_iota(jnp.int32, (64, 16), 0) & 7
    chosen = []
    for i in range(2):
        ends = [jnp.where(j_lane == 0, child[4 * i + l], child[4 * i + 2 + l]) for l in range(2)]
        chosen.append((slot_row == ends[0]) | (slot_row == ends[1]))

    def child_matrix(at):
        parts = [
            jnp.where(chosen[0], held["child_out"][4 * at + part], 0.0)
            + jnp.where(chosen[1], held["child_out"][4 * at + 2 + part], 0.0)
            for part in range(2)
        ]
        return [parts[0], parts[0], parts[1]]

    odd = lax.broadcasted_iota(jnp.int32, (8, 128), 0)
    odd = (odd == child[1]) | (odd == child[3]) | (odd == child[5]) | (odd == child[7])
    child_half = jnp.concatenate([odd == (half_lane == 1)] * 8, axis=0)

    def j_rows(plane):
        return jnp.concatenate([plane[:, :128], plane[:, 128:]], axis=0)

    def settle(array):
        array = jnp.where(child_half, array, 0.0)
        return array + turn(array)

    def to_flat(array):
        pairs = [jnp.where(low_lane, array[16 * k : 16 * k + 8], array[16 * k + 8 : 16 * k + 16]) for k in range(4)]
        return jnp.concatenate(pairs, axis=1)

    steps = [(c // 9 - 1, c // 3 % 3 - 1, c % 3 - 1) for c in range(27)]

    def inside(step):
        tests = []
        for at, size, move in zip(here, sizes, step):
            if move == 1:
                tests.append(at < size - 1)
            elif move == -1:
                tests.append(at > 0)
        found = tests[0]
        for test in tests[1:]:
            found = found & test
        return found

    def halo_copy(cell):
        peer = tuple(at + part for at, part in zip(here, steps[cell]))
        return pltpu.make_async_remote_copy(
            src_ref=halo.at[CENTRE],
            dst_ref=halo.at[26 - cell],
            send_sem=halo_send.at[cell],
            recv_sem=halo_recv.at[26 - cell],
            device_id=peer,
            device_id_type=MESH,
        )

    def to_all(buffer, send, recv):
        each_peer(lambda peer: pltpu.make_async_remote_copy(
            src_ref=buffer.at[me],
            dst_ref=buffer.at[me],
            send_sem=send.at[0],
            recv_sem=recv.at[0],
            device_id=peer,
            device_id_type=MESH,
        ).start())

    others = [cell for cell in range(27) if cell != CENTRE]

    def meet_and_send():
        pl.semaphore_wait(barrier, devices - 1)
        to_all(codes, code_send, code_recv)
        to_all(rows, row_send, row_recv)

    def build_tables():
        ready("op_factor", "term_weight", "spread", "swap", "widen")
        factor = loaded["op_factor"]
        planes = []
        for level in range(levels):
            for e in range(3):
                planes.append(jnp.concatenate([factor[level, e, b] for b in range(8)], axis=1))
        plane = jnp.concatenate(planes, axis=0)
        weight = jnp.concatenate([loaded["term_weight"][...]] * 8, axis=1)
        rounded = plane.astype(BF16)
        left_side = stack_halves(plane * weight).astype(F32)
        right_side = stack_halves(plane).astype(F32)
        count = plane.shape[0]
        group = 64 * QUAD
        for at in range(terms // QUAD):
            for side, first, factors in ((left_side, 0, factor_left), (right_side, group, factor_right)):
                some = pltpu.roll(side, 8 * terms - QUAD * at, 1) if at else side
                got = dot(some.astype(BF16), held["spread"][:, first : first + group])
                got = got[:count] + got[count:]
                factors[:, :, at * group : at * group + group] = got.reshape(levels * 3, 8, group)
        turned = dot_rows(held["swap"][...], rounded)
        for level in range(1, levels):
            parts = [turned[32 * at : 32 * at + 32, 24 * level : 24 * level + 24] for at in range(terms // QUAD)]
            mixers[level - 1] = jnp.concatenate(parts, axis=1).astype(BF16)
        mixers_t[...] = dot(turned.astype(BF16), held["widen"][...])

        def table_step(at, carry):
            level, ey = at // 3, at % 3
            left = factor_left.at[at]
            for ez in range(3):
                right = factor_right[level * 3 + ez]
                base = (ey * 3 + ez) * 64
                for k in range(4):
                    pair = [left[2 * k + half : 2 * k + half + 1, :] * right for half in range(2)]
                    start = pl.multiple_of(base + 16 * k, 16)
                    tables[level, pl.ds(start, 16), :] = jnp.concatenate(pair, axis=0).astype(BF16)
            return carry

        lax.fori_loop(0, levels * 3, table_step, 0)
        own_lane = (lanes((8, 192)) & 7) == lax.broadcasted_iota(jnp.int32, (8, 192), 0)

        for at in range(terms // 2):
            some = mixers_t[16 * at : 16 * at + 16, :]
            some = jnp.where(own_lane[None], jnp.broadcast_to(some[:, None, :], (16, 8, 192)), 0.0)
            part, first, lane = at // (2 * GROUPS), 128 * (at % 2), 192 * (at // 2 % GROUPS)
            block_mix[part, first : first + 128, lane : lane + 192] = some.reshape(128, 192).astype(BF16)

    away = lax.shift_right_logical(here[0], 1) + here[1] + here[2]
    far = 2 * away > (size_x - 1) // 2 + size_y + size_z - 2
    near_start = away <= EARLY

    @pl.when(far)
    def _():
        meet_and_send()

    own_matrix = child_matrix(0)
    plane = dot(placed, held["open"][...])
    plane = plane[:, :256] + plane[:, 256:]
    fine_from = dot(jnp.concatenate(own_matrix, axis=1).astype(BF16), triple(j_rows(plane)).astype(BF16))
    detail = live * (by_row - settle(fine_from))
    halo[CENTRE] = to_flat(detail).astype(BF16)

    for cell in others:
        @pl.when(jnp.logical_not(inside(steps[cell])))
        def _(cell=cell):
            halo[cell] = jnp.zeros(halo.shape[1:], BF16)

    @pl.when(near_start)
    def _():
        build_tables()

    @pl.when(jnp.logical_not(far))
    def _():
        meet_and_send()

    for cell in others:
        @pl.when(inside(steps[cell]))
        def _(cell=cell):
            halo_copy(cell).start()

    @pl.when(jnp.logical_not(near_start))
    def _():
        build_tables()

    ready("cells", "fine_nbr")
    cells = held["cells"]
    spot = [here[k] + cells[k : k + 1, :] for k in range(3)]
    there = None
    for k in range(3):
        test = (spot[k] >= 0) & (spot[k] < sizes[k])
        there = test if there is None else there & test
    names_row = ((spot[0] * size_y + spot[1]) * size_z + spot[2]) * 8 + cells[3:4, :]
    names_row = jnp.where(there, names_row, -2)
    near = loaded["fine_nbr"][...]
    hot = [(near[:, d : d + 1] == names_row).astype(F32) for d in range(27)]
    picks[...] = jnp.concatenate(hot, axis=0).astype(BF16)

    ready("mid_in", "mid_out", "own_out", "mid_nbr", "coarse_nbr", "coarse", "mid_tail", "coarse_tail")
    after_matrix = [jnp.where(my_octant >= 4, upper, lower)
                    for lower, upper in zip(child_matrix(1), child_matrix(2))]
    last_matrix = jnp.concatenate(own_matrix + after_matrix, axis=1).astype(BF16)
    own_out = jnp.where(my_octant >= 4, held["own_out"][1], held["own_out"][0]).astype(BF16)

    def arrived(buffer, sem):
        span = buffer.at[pl.ds(0, devices - 1)]
        return pltpu.make_async_copy(span, span, sem.at[0])

    arrived(codes, code_recv).wait()
    code = [
        jnp.sum(codes[first : min(first + 16, devices)], axis=0)[0:1] for first in range(0, devices, 16)
    ]
    code = jnp.concatenate(code, axis=1)[:, : devices * 8].astype(jnp.int32) - 1
    key = lax.shift_right_arithmetic(jnp.broadcast_to(code, (8, devices * 8)), 1)
    near_id = [loaded["mid_nbr"][0, d] for d in range(27)]
    near_code = []
    for named in near_id:
        got = codes[jnp.maximum(named, 0)][1:2, :].astype(jnp.int32)
        near_code.append(jnp.broadcast_to(jnp.where(named >= 0, got, 0) - 1, (8, 128)))
    batch_lane = lax.shift_right_logical(lanes((8, batch * 8)), 3)

    def choose_in(first):
        blocks = []
        for part in range(2):
            for k in range(batch):
                for j in range(2):
                    want = (first + k) * 4 + j
                    block = jnp.where(key == want, held["mid_in"][part], 0.0)
                    blocks.append(block + jnp.where(key == want + 2, held["mid_in"][2 + part], 0.0))
        return jnp.concatenate(blocks, axis=0).astype(BF16)

    def choose_out(first):
        lane_key = (first + batch_lane) * 2
        parts = [[], []]
        for d in range(27):
            mine = lax.shift_right_arithmetic(near_code[d][:, : batch * 8], 2)
            lower, upper = mine == lane_key, mine == lane_key + 1
            for part in range(2):
                block = jnp.where(lower, held["mid_out"][part], 0.0)
                parts[part].append(block + jnp.where(upper, held["mid_out"][2 + part], 0.0))
        parts = [jnp.concatenate(part, axis=0) for part in parts]
        return jnp.concatenate([parts[0], parts[0], parts[1]], axis=1).astype(BF16)

    batches = coarse // batch
    if batches == 1:
        first_in, first_out = choose_in(0), choose_out(0)

    for cell in others:
        @pl.when(inside(steps[cell]))
        def _(cell=cell):
            halo_copy(26 - cell).wait_recv()
    got = dot(picks[...], halo[...].astype(F32).reshape(216, 512).astype(BF16))
    blocks = []
    for ex in range(3):
        here_rows = [got[(ex * 9 + e) * 8 : (ex * 9 + e) * 8 + 8] for e in range(9)]
        for k in range(4):
            tile = [part[:, 128 * k : 128 * k + 128] for part in here_rows]
            turned = [turn(part) for part in tile]
            even = [jnp.where(low_lane, tile[e], turned[e + 1]) for e in range(0, 8, 2)]
            uneven = [jnp.where(low_lane, turned[e], tile[e + 1]) for e in range(0, 8, 2)]
            blocks.append(jnp.concatenate(even + [tile[8][:, :64]], axis=1))
            blocks.append(jnp.concatenate(uneven + [turned[8][:, :64]], axis=1))
    fine_sources = jnp.concatenate(blocks, axis=0).astype(BF16)
    fine_total = []

    def spread_fine(at):
        spread = dot(fine_sources, tables[0, :, at * 256 : at * 256 + 256])
        spreads[192 * at : 192 * at + 192, :] = spread.astype(BF16)

    def mix_fine(part):
        rows_of = 192 * GROUPS
        fine_total.append(dot(block_mix[part], spreads[rows_of * part : rows_of * part + rows_of, :]))

    fine_work = []
    for at in range(terms // QUAD):
        fine_work.append(lambda at=at: spread_fine(at))
        if at >= GROUPS and at % GROUPS == 0:
            fine_work.append(lambda part=at // GROUPS - 1: mix_fine(part))
    fine_work.append(lambda: mix_fine(terms // QUAD // GROUPS - 1))
    fine_work = iter(fine_work)

    def fine_step(count=1):
        for _, work in zip(range(count), fine_work):
            work()

    arrived(rows, row_recv).wait()
    gathered = rows[...].astype(F32).reshape(devices * 8, 128).astype(BF16)

    def coarse_step(at, total, chosen_in, chosen_out, between=lambda: None):
        mixed = dot(chosen_in, gathered)
        between()
        mixed = mixed[: batch * 16] + mixed[batch * 16 :]
        wide = [
            jnp.concatenate([mixed[16 * k : 16 * k + 8], mixed[16 * k + 8 : 16 * k + 16]], axis=1)
            for k in range(batch)
        ]
        got = dot(stack_halves(jnp.concatenate(wide, axis=0)), held["coarse"][...])
        between()
        top = batch * 8
        plane = got[:top, 256:512] + got[:top, 512:] + got[top:, 256:512]
        source = got[:top, :128] + got[:top, 128:256] + got[top:, :128]
        coarse_tab[pl.ds(at * batch, batch)] = source.reshape(batch, 8, 128)
        found = dot(chosen_out, triple(plane).astype(BF16))
        return found if total is None else total + found

    zero = jnp.zeros((216, 256), F32)
    if batches == 1:
        from_coarse = coarse_step(0, None, first_in, first_out, fine_step)
    else:
        from_coarse = lax.fori_loop(
            0, batches,
            lambda at, total: coarse_step(at, total, choose_in(at * batch), choose_out(at * batch)), zero)

    def pair_up(blocks):
        pairs = [jnp.where(low_lane, blocks[e], blocks[e + 1]) for e in range(0, 8, 2)]
        return jnp.concatenate(pairs + [blocks[8][:, :64]], axis=1)

    coarse_blocks = []
    for ex in range(3):
        got = []
        for e in range(9):
            named = loaded["coarse_nbr"][my_parent, ex * 9 + e]
            got.append(jnp.where(named >= 0, coarse_tab[jnp.maximum(named, 0)], 0.0))
        coarse_blocks.append(pair_up(got))
    coarse_sources = jnp.concatenate(coarse_blocks, axis=0).astype(BF16)
    quad_lane = lax.shift_right_logical(lanes((8, 256)), 6)

    def spread_one(level, sources):
        return dot(sources, tables[level])

    def mix_one(level, spread):
        parts = [spread[:, at * 256 : at * 256 + 256] for at in range(terms // QUAD)]
        total = dot(mixers[level - 1], jnp.concatenate(parts, axis=0).astype(BF16))
        fine_step()
        result = jnp.where(quad_lane == 0, total[:8], 0.0)
        for k in range(1, QUAD):
            result = jnp.where(quad_lane == k, total[8 * k : 8 * k + 8], result)
        return result[:, :128] + result[:, 128:]

    coarse_spread = spread_one(2, coarse_sources)
    near_blocks = []
    for d in range(27):
        tile = jnp.where(near_id[d] >= 0, rows[jnp.maximum(near_id[d], 0)].astype(F32), 0.0)
        part = from_coarse[8 * d : 8 * d + 8]
        part = jnp.where((near_code[d] & 2) > 0, part[:, 128:], part[:, :128])
        tile = tile - jnp.where(half_lane == (near_code[d] & 1), part, 0.0)
        near_blocks.append(tile + turn(tile))
    mid_sources = [pair_up(near_blocks[9 * ex : 9 * ex + 9]) for ex in range(3)]
    mid_sources = jnp.concatenate(mid_sources, axis=0).astype(BF16)
    mid_spread = spread_one(1, mid_sources)
    coarse_raw = mix_one(2, coarse_spread)
    tail = dot(stack_halves(coarse_raw), held["coarse_tail"][my_octant & 3])
    fine_step()
    mid_raw = mix_one(1, mid_spread)
    got = tail
    mine = got[:8, :128] + got[:8, 128:256] + got[8:, :128]
    coarse_plane = got[:8, 256:512] + got[:8, 512:] + got[8:, 256:512]
    tail = dot(stack_halves(mid_raw), held["mid_tail"][...])
    from_above = dot(own_out, triple(mine).astype(BF16))
    fine_step()
    got = tail
    mid_plane = got[:8, 128:384] + got[:8, 384:] + got[8:, 128:384]
    planes = jnp.concatenate([triple(j_rows(mid_plane)), triple(j_rows(coarse_plane))], axis=0)
    fine_from = dot(last_matrix, planes.astype(BF16))
    fine_step(3 * terms)
    fine_from = settle(fine_from)
    mid_out = got[:8, :128] + got[8:, :128] + from_above
    for a in range(8):
        at = 64 * (a % 2)
        mid_ref[0:1, 64 * a : 64 * a + 64] = mid_out[a : a + 1, at : at + 64]

    total = sum(fine_total[1:], fine_total[0])
    direct = []
    for a in range(8):
        part = jnp.where(quad_lane == 0, total[8 * a : 8 * a + 8], 0.0)
        for k in range(1, QUAD):
            part = jnp.where(quad_lane == k, total[64 * k + 8 * a : 64 * k + 8 * a + 8], part)
        direct.append(part[:, :128] + part[:, 128:])
    direct = jnp.concatenate(direct, axis=0)
    direct = direct + turn(direct)
    fine_ref[...] = to_flat(live * (direct + fine_from))

    arrived(codes, code_send).wait()
    arrived(rows, row_send).wait()
    for cell in others:
        @pl.when(inside(steps[cell]))
        def _(cell=cell):
            halo_copy(cell).wait_send()


SCALARS = ("mid_child", "mid_parent", "mid_refined", "mid_nbr", "coarse_nbr")


def shards(sizes, fine_coef, mid_leaf, mid_child, mid_parent, mid_refined, fine_nbr, mid_nbr, coarse_nbr,
           op_factor, term_weight):
    levels, terms = op_factor.shape[:2]
    coarse = coarse_nbr.shape[0]
    devices = math.prod(sizes)
    batch = math.gcd(coarse, 4)
    assert mid_child.shape == (1, 8) and fine_coef.shape == (8, 512) and terms % QUAD == 0
    args = dict(
        mid_child=mid_child, mid_parent=mid_parent, mid_refined=mid_refined, fine_coef=fine_coef,
        mid_leaf=mid_leaf, fine_nbr=fine_nbr, mid_nbr=mid_nbr, coarse_nbr=coarse_nbr,
        op_factor=jnp.transpose(op_factor, (0, 2, 3, 4, 1)), term_weight=term_weight[None, :],
    )
    consts = {name: jnp.asarray(value) for name, value in constants(terms, devices, batch).items()}
    arg_names, const_names = list(args), list(consts)
    dma = pltpu.SemaphoreType.DMA
    width = 64 * terms

    def buffer(name, value):
        space = pltpu.SMEM if name in SCALARS else pltpu.VMEM
        return space(value.shape, value.dtype)

    scratch = [buffer(name, value) for name, value in args.items()]
    scratch += [buffer(name, value) for name, value in consts.items()]
    scratch += [
        pltpu.VMEM((27, 8, 512), BF16),
        pltpu.VMEM((devices, 8, 128), BF16),
        pltpu.VMEM((devices, 2, 128), F32),
        pltpu.VMEM((levels * 3, 8, width), F32),
        pltpu.VMEM((levels * 3, 8, width), F32),
        pltpu.VMEM((levels, 576, width), BF16),
        pltpu.VMEM((levels - 1, 8 * QUAD, 24 * (terms // QUAD)), BF16),
        pltpu.VMEM((8 * terms, 192), F32),
        pltpu.VMEM((terms // QUAD // GROUPS, 64 * QUAD, 192 * GROUPS), BF16),
        pltpu.VMEM((192 * (terms // QUAD), 64 * QUAD), BF16),
        pltpu.VMEM((216, 216), BF16),
        pltpu.VMEM((coarse, 8, 128), F32),
        dma((len(args),)), dma((len(consts),)), dma((1,)), dma((1,)), dma((1,)), dma((1,)), dma((27,)), dma((27,)),
    ]

    def body(*refs):
        n_args, n_consts = len(arg_names), len(const_names)
        ins, refs = refs[: n_args + n_consts], refs[n_args + n_consts :]
        outs, refs = refs[:2], refs[2:]
        loaded = dict(zip(arg_names, refs[:n_args]))
        held = dict(zip(const_names, refs[n_args : n_args + n_consts]))
        kernel(sizes, batch, levels, terms, coarse, dict(zip(arg_names, ins[:n_args])),
               dict(zip(const_names, ins[n_args:])), outs, (loaded, held) + tuple(refs[n_args + n_consts :]))

    vmem = pl.BlockSpec(memory_space=pltpu.VMEM)
    hbm = pl.BlockSpec(memory_space=pltpu.HBM)
    shapes = ((8, 512), (1, 512))
    inner = pl.pallas_call(
        body,
        out_shape=tuple(pltpu.VMEM(shape, F32) for shape in shapes),
        in_specs=[hbm] * (len(args) + len(consts)),
        out_specs=(vmem, vmem),
        scratch_shapes=scratch,
        compiler_params=pltpu.CompilerParams(
            collective_id=0, has_side_effects=True, vmem_limit_bytes=58 * 1024 * 1024),
        name="tree",
    )(*args.values(), *consts.values())

    def store(fine_in, mid_in, fine_to, mid_to, sem):
        copies = [
            pltpu.make_async_copy(fine_in, fine_to, sem.at[0]),
            pltpu.make_async_copy(mid_in, mid_to, sem.at[1]),
        ]
        for copy in copies:
            copy.start()
        for copy in copies:
            copy.wait()

    return pl.pallas_call(
        store,
        out_shape=tuple(jax.ShapeDtypeStruct(shape, F32) for shape in shapes),
        in_specs=[pl.BlockSpec(memory_space=pl.ANY)] * 2,
        out_specs=(hbm, hbm),
        scratch_shapes=[dma((2,))],
        compiler_params=pltpu.CompilerParams(vmem_limit_bytes=1 << 20),
        name="store",
    )(*inner)


def solution(mesh):
    sizes = tuple(mesh.shape[axis] for axis in AXES)
    split = P(AXES, None)
    line = P(AXES)
    return jax.shard_map(
        lambda *args: shards(sizes, *args),
        mesh=mesh,
        in_specs=(split, split, split, line, line, split, split, P(), P(), P()),
        out_specs=(split, split),
        check_vma=False,
    )
```

```python
import math

import jax
import jax.numpy as jnp
import numpy as np
from jax import lax
from jax.experimental import pallas as pl
from jax.experimental.pallas import tpu as pltpu
from jax.sharding import PartitionSpec as P

MESH = pl.DeviceIdType.MESH
AXES = ("gx", "gy", "gz")
CENTRE = 13
QUAD = 4
EARLY = 1
GROUPS = 4
F32 = jnp.float32
BF16 = jnp.bfloat16


def poly_multiply(left, right):
    result = [0.0] * (len(left) + len(right) - 1)
    for first, left_coef in enumerate(left):
        for second, right_coef in enumerate(right):
            result[first + second] += left_coef * right_coef
    return result


def poly_compose(coeffs, factor, offset):
    result = [0.0]
    power_term = [1.0]
    for coef in coeffs:
        padded = result + [0.0] * (len(power_term) - len(result))
        result = [padded[place] + coef * power_term[place] for place in range(len(power_term))]
        power_term = poly_multiply(power_term, [offset, factor])
    return result


def legendre_table(basis_order):
    polys = [[1.0], [0.0, 1.0]]
    for degree in range(1, basis_order):
        upper = [0.0] + [(2 * degree + 1) * coef for coef in polys[degree]]
        lower = [degree * coef for coef in polys[degree - 1]] + [0.0] * (
            len(upper) - len(polys[degree - 1])
        )
        polys.append([(upper[place] - lower[place]) / (degree + 1) for place in range(len(upper))])
    return [
        [math.sqrt(2 * degree + 1) * coef for coef in poly_compose(polys[degree], 2.0, -1.0)]
        for degree in range(basis_order)
    ]


def two_scale(basis_order):
    shifted = legendre_table(basis_order)
    filters = np.zeros((2, basis_order, basis_order))
    for which_half in range(2):
        for row_at in range(basis_order):
            halved = poly_compose(shifted[row_at], 0.5, 0.5 * which_half)
            for col_at in range(basis_order):
                product = poly_multiply(halved, shifted[col_at])
                total = sum((coef / (place + 1) for place, coef in enumerate(product)))
                filters[which_half, row_at, col_at] = total / math.sqrt(2.0)
    return np.asarray(filters, np.float32)


def halves(array):
    high = array.astype(BF16)
    return high, (array - high.astype(array.dtype)).astype(BF16)


def np_halves(array):
    array = np.asarray(array, np.float32)
    high = array.astype(BF16)
    return high, (array - high.astype(np.float32)).astype(BF16)


def dot(left, right):
    return jnp.dot(left, right, preferred_element_type=F32)


def dot_rows(left, right):
    return lax.dot_general(left, right, (((1,), (1,)), ((), ())), preferred_element_type=F32)


def constants(terms, devices, batch):
    filters = two_scale(8)
    exact = np.asarray(filters, np.float64)
    table = {}
    row = np.arange(8 * terms)
    lane = np.arange(64 * QUAD)
    same = (row % terms)[:, None] == (lane // 64)[None, :]
    spread = [same & ((row // terms)[:, None] == part[None, :]) for part in (lane // 8 % 8, lane % 8)]
    table["spread"] = np.concatenate(spread, axis=1).astype(BF16)
    swap = (row // 8)[:, None] == (row % terms)[None, :]
    swap &= (row % 8)[:, None] == (row // terms)[None, :]
    table["swap"] = swap.astype(BF16)
    table["widen"] = (np.arange(72)[:, None] == (np.arange(192) // 8)[None, :]).astype(BF16)
    close = np.einsum("jqy,lrz->jlyzqr", exact, exact).reshape(256, 64)
    opened = np.ascontiguousarray(close.T)
    twice = np.concatenate([close, close], axis=1)
    table["close"] = np.concatenate(np_halves(twice), axis=1)
    table["open"] = np.concatenate([np.concatenate(np_halves(opened), axis=1)] * 2, axis=0)
    table["coarse"] = np.concatenate(np_halves(twice) + np_halves(close @ opened), axis=1)
    fold = np.tile(np.eye(64, dtype=np.float32), (2, 2)).astype(BF16)
    stack = np.tile(opened, (2, 1))
    table["mid_tail"] = np.concatenate((fold,) + np_halves(stack), axis=1)
    tails = []
    for jl in range(4):
        mine = opened[:, 64 * jl : 64 * jl + 64]
        both = np.tile(np.concatenate([mine, mine], axis=1), (2, 1))
        tails.append(np.concatenate(np_halves(both) + np_halves(np.tile(mine @ opened, (2, 1))), axis=1))
    table["coarse_tail"] = np.stack(tails)
    parts = [np.asarray(part, np.float32) for part in np_halves(filters)]
    both = np.stack(parts, axis=1).reshape(4, 8, 8)
    flip = np.swapaxes(both, 1, 2)
    table["child_in"] = np.repeat(both, 8, axis=2)
    chains = [[exact[i].T for i in range(2)]]
    chains += [[exact[i].T @ exact[own].T for i in range(2)] for own in range(2)]
    out = np.stack([np.stack(np_halves(chain)) for chain_set in chains for chain in chain_set])
    out = np.asarray(out, np.float32).reshape(12, 8, 8)
    table["child_out"] = np.tile(np.repeat(out, 8, axis=1), (1, 1, 2))
    table["mid_in"] = np.tile(both, (1, 1, devices))
    table["mid_out"] = np.tile(flip, (1, 1, batch))
    own = [np.concatenate([flip[2 * i], flip[2 * i], flip[2 * i + 1]], axis=1) for i in range(2)]
    table["own_out"] = np.stack(own)
    cell = np.arange(27 * 8) // 8
    cells = np.zeros((8, 27 * 8), np.int32)
    cells[:4] = np.stack([cell // 9 - 1, cell // 3 % 3 - 1, cell % 3 - 1, np.arange(27 * 8) % 8])
    table["cells"] = cells
    return table


def kernel(sizes, batch, levels, terms, coarse, args, consts, outs, scratch):
    size_x, size_y, size_z = sizes
    devices = size_x * size_y * size_z
    here = [lax.axis_index(axis) for axis in AXES]
    me = (here[0] * size_y + here[1]) * size_z + here[2]
    fine_ref, mid_ref = outs
    (loaded, held, halo, rows, codes, factor_left, factor_right, tables, mixers, mixers_t, block_mix, spreads, picks,
     coarse_tab, load_sem, held_sem, row_send, row_recv, code_send, code_recv, halo_send, halo_recv) = scratch

    spots = [(x, y, z) for x in range(size_x) for y in range(size_y) for z in range(size_z)]
    spots.sort(key=lambda spot: spot[0] // 2 + spot[1] + spot[2])
    front = [spot for spot in spots if spot[0] // 2 + spot[1] + spot[2] <= EARLY]
    unrolled = devices <= 64

    def each_peer(body, chosen=spots):
        if unrolled:
            for spot in chosen:
                @pl.when(me != (spot[0] * size_y + spot[1]) * size_z + spot[2])
                def _(spot=spot):
                    body(spot)
        else:
            def step(offset, carry):
                device = lax.rem(me + offset, devices)
                body((device // (size_y * size_z), device // size_z % size_y, device % size_z))
                return carry
            lax.fori_loop(1, devices, step, 0)

    loads = {}
    for at, (name, source) in enumerate(args.items()):
        loads[name] = pltpu.make_async_copy(source, loaded[name], load_sem.at[at])
    for at, (name, source) in enumerate(consts.items()):
        loads[name] = pltpu.make_async_copy(source, held[name], held_sem.at[at])
    order = ["mid_child", "mid_parent", "mid_refined", "fine_coef", "mid_leaf", "child_in", "close",
             "child_out", "open"]
    order += [name for name in loads if name not in order]
    for name in order[:9]:
        loads[name].start()
    barrier = pltpu.get_barrier_semaphore()
    each_peer(lambda peer: pl.semaphore_signal(
        barrier, inc=1, device_id=peer, device_id_type=MESH))
    for name in order[9:]:
        loads[name].start()

    def ready(*wanted):
        for name in wanted:
            loads[name].wait()

    def turn(array):
        return pltpu.roll(array, 64, 1)

    def lanes(shape):
        return lax.broadcasted_iota(jnp.int32, shape, len(shape) - 1)

    def stack_halves(array):
        high, low = halves(array)
        return jnp.concatenate([high.astype(F32), low.astype(F32)], axis=0).astype(BF16)

    def triple(array):
        high, low = halves(array)
        high, low = high.astype(F32), low.astype(F32)
        return jnp.concatenate([high, low, high], axis=0)

    half_lane = lax.shift_right_logical(lanes((8, 128)), 6)
    low_lane = half_lane == 0

    ready("mid_child", "mid_parent", "mid_refined", "fine_coef", "mid_leaf", "child_in", "close")
    child = [loaded["mid_child"][0, o] for o in range(8)]
    refined = loaded["mid_refined"][0] > 0
    live = jnp.where(refined, 1.0, 0.0).astype(F32)
    mid_parent = loaded["mid_parent"][0]
    my_parent = lax.shift_right_logical(mid_parent, 3)
    my_octant = mid_parent & 7
    code_lane = lax.shift_right_logical(lanes((2, 128)), 3) == (me & 15)
    code_row = lax.broadcasted_iota(jnp.int32, (2, 128), 0) == 1
    codes[me] = jnp.where(code_lane | code_row, mid_parent + 1, 0).astype(F32)

    flat = loaded["fine_coef"][...].astype(F32)
    by_row = []
    for k in range(4):
        tile = flat[:, 128 * k : 128 * k + 128]
        turned = turn(tile)
        by_row += [jnp.where(low_lane, tile, turned), jnp.where(low_lane, turned, tile)]
    by_row = jnp.concatenate(by_row, axis=0)
    slot_lane = lanes((8, 64)) & 7
    child_in = [held["child_in"][k] for k in range(4)]
    blocks = []
    for part in range(2):
        for jl in range(4):
            block = jnp.where(slot_lane == child[jl], child_in[part], 0.0)
            blocks.append(block + jnp.where(slot_lane == child[4 + jl], child_in[2 + part], 0.0))
    mixed = dot(jnp.concatenate(blocks, axis=0).astype(BF16), by_row.astype(BF16))
    mixed = mixed[:32] + mixed[32:]
    wide = [jnp.where(low_lane, mixed[16 * j : 16 * j + 8], mixed[16 * j + 8 : 16 * j + 16]) for j in range(2)]
    got = dot(stack_halves(jnp.concatenate(wide, axis=1)), held["close"][...])
    compressed = got[:8, :128] + got[:8, 128:] + got[8:, :128]
    leaf = jnp.broadcast_to(loaded["mid_leaf"][...].astype(F32), (8, 512))
    leaf_block = lax.shift_right_logical(lanes((8, 512)), 6)
    leaf = jnp.where(leaf_block == lax.broadcasted_iota(jnp.int32, (8, 512), 0), leaf, 0.0)
    leaf = leaf[:, :128] + leaf[:, 128:256] + leaf[:, 256:384] + leaf[:, 384:]
    leaf = leaf + turn(leaf)
    mid_source = jnp.where(refined, compressed, leaf)
    placed = jnp.where(half_lane == (my_octant & 1), mid_source, 0.0).astype(BF16)
    rows[me] = placed

    ready("child_out", "open")
    j_lane = lax.shift_right_logical(lanes((64, 16)), 3)
    slot_row = lax.broadcasted_iota(jnp.int32, (64, 16), 0) & 7
    chosen = []
    for i in range(2):
        ends = [jnp.where(j_lane == 0, child[4 * i + l], child[4 * i + 2 + l]) for l in range(2)]
        chosen.append((slot_row == ends[0]) | (slot_row == ends[1]))

    def child_matrix(at):
        parts = [
            jnp.where(chosen[0], held["child_out"][4 * at + part], 0.0)
            + jnp.where(chosen[1], held["child_out"][4 * at + 2 + part], 0.0)
            for part in range(2)
        ]
        return [parts[0], parts[0], parts[1]]

    odd = lax.broadcasted_iota(jnp.int32, (8, 128), 0)
    odd = (odd == child[1]) | (odd == child[3]) | (odd == child[5]) | (odd == child[7])
    child_half = jnp.concatenate([odd == (half_lane == 1)] * 8, axis=0)

    def j_rows(plane):
        return jnp.concatenate([plane[:, :128], plane[:, 128:]], axis=0)

    def settle(array):
        array = jnp.where(child_half, array, 0.0)
        return array + turn(array)

    def to_flat(array):
        pairs = [jnp.where(low_lane, array[16 * k : 16 * k + 8], array[16 * k + 8 : 16 * k + 16]) for k in range(4)]
        return jnp.concatenate(pairs, axis=1)

    steps = [(c // 9 - 1, c // 3 % 3 - 1, c % 3 - 1) for c in range(27)]

    def inside(step):
        tests = []
        for at, size, move in zip(here, sizes, step):
            if move == 1:
                tests.append(at < size - 1)
            elif move == -1:
                tests.append(at > 0)
        found = tests[0]
        for test in tests[1:]:
            found = found & test
        return found

    def halo_copy(cell):
        peer = tuple(at + part for at, part in zip(here, steps[cell]))
        return pltpu.make_async_remote_copy(
            src_ref=halo.at[CENTRE],
            dst_ref=halo.at[26 - cell],
            send_sem=halo_send.at[cell],
            recv_sem=halo_recv.at[26 - cell],
            device_id=peer,
            device_id_type=MESH,
        )

    def send_code(peer):
        pltpu.make_async_remote_copy(
            src_ref=codes.at[me],
            dst_ref=codes.at[me],
            send_sem=code_send.at[0],
            recv_sem=code_recv.at[0],
            device_id=peer,
            device_id_type=MESH,
        ).start()

    def send_row(peer):
        pltpu.make_async_remote_copy(
            src_ref=rows.at[me],
            dst_ref=rows.at[me],
            send_sem=row_send.at[0],
            recv_sem=row_recv.at[0],
            device_id=peer,
            device_id_type=MESH,
        ).start()

    def send_both(peer):
        send_code(peer)
        send_row(peer)

    others = [cell for cell in range(27) if cell != CENTRE]

    def meet_and_send():
        pl.semaphore_wait(barrier, devices - 1)
        if unrolled:
            each_peer(send_both, front)
            each_peer(send_code, spots[len(front) :])
            each_peer(send_row, spots[len(front) :])
        else:
            each_peer(send_both)

    def build_tables():
        ready("op_factor", "term_weight", "spread", "swap", "widen")
        factor = loaded["op_factor"]
        planes = []
        for level in range(levels):
            for e in range(3):
                planes.append(jnp.concatenate([factor[level, e, b] for b in range(8)], axis=1))
        plane = jnp.concatenate(planes, axis=0)
        weight = jnp.concatenate([loaded["term_weight"][...]] * 8, axis=1)
        rounded = plane.astype(BF16)
        left_side = stack_halves(plane * weight).astype(F32)
        right_side = stack_halves(plane).astype(F32)
        count = plane.shape[0]
        group = 64 * QUAD
        for at in range(terms // QUAD):
            for side, first, factors in ((left_side, 0, factor_left), (right_side, group, factor_right)):
                some = pltpu.roll(side, 8 * terms - QUAD * at, 1) if at else side
                got = dot(some.astype(BF16), held["spread"][:, first : first + group])
                got = got[:count] + got[count:]
                factors[:, :, at * group : at * group + group] = got.reshape(levels * 3, 8, group)
        turned = dot_rows(held["swap"][...], rounded)
        for level in range(1, levels):
            parts = [turned[32 * at : 32 * at + 32, 24 * level : 24 * level + 24] for at in range(terms // QUAD)]
            mixers[level - 1] = jnp.concatenate(parts, axis=1).astype(BF16)
        mixers_t[...] = dot(turned.astype(BF16), held["widen"][...])

        def table_step(at, carry):
            level, ey = at // 3, at % 3
            left = factor_left.at[at]
            for ez in range(3):
                right = factor_right[level * 3 + ez]
                base = (ey * 3 + ez) * 64
                for k in range(4):
                    pair = [left[2 * k + half : 2 * k + half + 1, :] * right for half in range(2)]
                    start = pl.multiple_of(base + 16 * k, 16)
                    tables[level, pl.ds(start, 16), :] = jnp.concatenate(pair, axis=0).astype(BF16)
            return carry

        lax.fori_loop(0, levels * 3, table_step, 0)
        own_lane = (lanes((8, 192)) & 7) == lax.broadcasted_iota(jnp.int32, (8, 192), 0)

        for at in range(terms // 2):
            some = mixers_t[16 * at : 16 * at + 16, :]
            some = jnp.where(own_lane[None], jnp.broadcast_to(some[:, None, :], (16, 8, 192)), 0.0)
            part, first, lane = at // (2 * GROUPS), 128 * (at % 2), 192 * (at // 2 % GROUPS)
            block_mix[part, first : first + 128, lane : lane + 192] = some.reshape(128, 192).astype(BF16)

    away = lax.shift_right_logical(here[0], 1) + here[1] + here[2]
    far = 2 * away > (size_x - 1) // 2 + size_y + size_z - 2
    near_start = away <= EARLY

    @pl.when(far)
    def _():
        meet_and_send()

    own_matrix = child_matrix(0)
    plane = dot(placed, held["open"][...])
    plane = plane[:, :256] + plane[:, 256:]
    fine_from = dot(jnp.concatenate(own_matrix, axis=1).astype(BF16), triple(j_rows(plane)).astype(BF16))
    detail = live * (by_row - settle(fine_from))
    halo[CENTRE] = to_flat(detail).astype(BF16)

    for cell in others:
        @pl.when(jnp.logical_not(inside(steps[cell])))
        def _(cell=cell):
            halo[cell] = jnp.zeros(halo.shape[1:], BF16)

    @pl.when(near_start)
    def _():
        build_tables()

    @pl.when(jnp.logical_not(far))
    def _():
        meet_and_send()

    for cell in others:
        @pl.when(inside(steps[cell]))
        def _(cell=cell):
            halo_copy(cell).start()

    @pl.when(jnp.logical_not(near_start))
    def _():
        build_tables()

    ready("cells", "fine_nbr")
    cells = held["cells"]
    spot = [here[k] + cells[k : k + 1, :] for k in range(3)]
    there = None
    for k in range(3):
        test = (spot[k] >= 0) & (spot[k] < sizes[k])
        there = test if there is None else there & test
    names_row = ((spot[0] * size_y + spot[1]) * size_z + spot[2]) * 8 + cells[3:4, :]
    names_row = jnp.where(there, names_row, -2)
    near = loaded["fine_nbr"][...]
    hot = [(near[:, d : d + 1] == names_row).astype(F32) for d in range(27)]
    picks[...] = jnp.concatenate(hot, axis=0).astype(BF16)

    ready("mid_in", "mid_out", "own_out", "mid_nbr", "coarse_nbr", "coarse", "mid_tail", "coarse_tail")
    after_matrix = [jnp.where(my_octant >= 4, upper, lower)
                    for lower, upper in zip(child_matrix(1), child_matrix(2))]
    last_matrix = jnp.concatenate(own_matrix + after_matrix, axis=1).astype(BF16)
    own_out = jnp.where(my_octant >= 4, held["own_out"][1], held["own_out"][0]).astype(BF16)

    def arrived(buffer, sem):
        span = buffer.at[pl.ds(0, devices - 1)]
        return pltpu.make_async_copy(span, span, sem.at[0])

    arrived(codes, code_recv).wait()
    code = [
        jnp.sum(codes[first : min(first + 16, devices)], axis=0)[0:1] for first in range(0, devices, 16)
    ]
    code = jnp.concatenate(code, axis=1)[:, : devices * 8].astype(jnp.int32) - 1
    key = lax.shift_right_arithmetic(jnp.broadcast_to(code, (8, devices * 8)), 1)
    near_id = [loaded["mid_nbr"][0, d] for d in range(27)]
    near_code = []
    for named in near_id:
        got = codes[jnp.maximum(named, 0)][1:2, :].astype(jnp.int32)
        near_code.append(jnp.broadcast_to(jnp.where(named >= 0, got, 0) - 1, (8, 128)))
    batch_lane = lax.shift_right_logical(lanes((8, batch * 8)), 3)

    def choose_in(first):
        blocks = []
        for part in range(2):
            for k in range(batch):
                for j in range(2):
                    want = (first + k) * 4 + j
                    block = jnp.where(key == want, held["mid_in"][part], 0.0)
                    blocks.append(block + jnp.where(key == want + 2, held["mid_in"][2 + part], 0.0))
        return jnp.concatenate(blocks, axis=0).astype(BF16)

    def choose_out(first):
        lane_key = (first + batch_lane) * 2
        parts = [[], []]
        for d in range(27):
            mine = lax.shift_right_arithmetic(near_code[d][:, : batch * 8], 2)
            lower, upper = mine == lane_key, mine == lane_key + 1
            for part in range(2):
                block = jnp.where(lower, held["mid_out"][part], 0.0)
                parts[part].append(block + jnp.where(upper, held["mid_out"][2 + part], 0.0))
        parts = [jnp.concatenate(part, axis=0) for part in parts]
        return jnp.concatenate([parts[0], parts[0], parts[1]], axis=1).astype(BF16)

    batches = coarse // batch
    if batches == 1:
        first_in, first_out = choose_in(0), choose_out(0)

    for cell in others:
        @pl.when(inside(steps[cell]))
        def _(cell=cell):
            halo_copy(26 - cell).wait_recv()
    got = dot(picks[...], halo[...].astype(F32).reshape(216, 512).astype(BF16))
    blocks = []
    for ex in range(3):
        here_rows = [got[(ex * 9 + e) * 8 : (ex * 9 + e) * 8 + 8] for e in range(9)]
        for k in range(4):
            tile = [part[:, 128 * k : 128 * k + 128] for part in here_rows]
            turned = [turn(part) for part in tile]
            even = [jnp.where(low_lane, tile[e], turned[e + 1]) for e in range(0, 8, 2)]
            uneven = [jnp.where(low_lane, turned[e], tile[e + 1]) for e in range(0, 8, 2)]
            blocks.append(jnp.concatenate(even + [tile[8][:, :64]], axis=1))
            blocks.append(jnp.concatenate(uneven + [turned[8][:, :64]], axis=1))
    fine_sources = jnp.concatenate(blocks, axis=0).astype(BF16)
    fine_total = []

    def spread_fine(at):
        spread = dot(fine_sources, tables[0, :, at * 256 : at * 256 + 256])
        spreads[192 * at : 192 * at + 192, :] = spread.astype(BF16)

    def mix_fine(part):
        rows_of = 192 * GROUPS
        fine_total.append(dot(block_mix[part], spreads[rows_of * part : rows_of * part + rows_of, :]))

    fine_work = []
    for at in range(terms // QUAD):
        fine_work.append(lambda at=at: spread_fine(at))
        if at >= GROUPS and at % GROUPS == 0:
            fine_work.append(lambda part=at // GROUPS - 1: mix_fine(part))
    fine_work.append(lambda: mix_fine(terms // QUAD // GROUPS - 1))
    fine_work = iter(fine_work)

    def fine_step(count=1):
        for _, work in zip(range(count), fine_work):
            work()

    arrived(rows, row_recv).wait()
    gathered = rows[...].astype(F32).reshape(devices * 8, 128).astype(BF16)

    def coarse_step(at, total, chosen_in, chosen_out, between=lambda: None):
        mixed = dot(chosen_in, gathered)
        between()
        mixed = mixed[: batch * 16] + mixed[batch * 16 :]
        wide = [
            jnp.concatenate([mixed[16 * k : 16 * k + 8], mixed[16 * k + 8 : 16 * k + 16]], axis=1)
            for k in range(batch)
        ]
        got = dot(stack_halves(jnp.concatenate(wide, axis=0)), held["coarse"][...])
        between()
        top = batch * 8
        plane = got[:top, 256:512] + got[:top, 512:] + got[top:, 256:512]
        source = got[:top, :128] + got[:top, 128:256] + got[top:, :128]
        coarse_tab[pl.ds(at * batch, batch)] = source.reshape(batch, 8, 128)
        found = dot(chosen_out, triple(plane).astype(BF16))
        return found if total is None else total + found

    zero = jnp.zeros((216, 256), F32)
    if batches == 1:
        from_coarse = coarse_step(0, None, first_in, first_out, fine_step)
    else:
        from_coarse = lax.fori_loop(
            0, batches,
            lambda at, total: coarse_step(at, total, choose_in(at * batch), choose_out(at * batch)), zero)

    def pair_up(blocks):
        pairs = [jnp.where(low_lane, blocks[e], blocks[e + 1]) for e in range(0, 8, 2)]
        return jnp.concatenate(pairs + [blocks[8][:, :64]], axis=1)

    coarse_blocks = []
    for ex in range(3):
        got = []
        for e in range(9):
            named = loaded["coarse_nbr"][my_parent, ex * 9 + e]
            got.append(jnp.where(named >= 0, coarse_tab[jnp.maximum(named, 0)], 0.0))
        coarse_blocks.append(pair_up(got))
    coarse_sources = jnp.concatenate(coarse_blocks, axis=0).astype(BF16)
    quad_lane = lax.shift_right_logical(lanes((8, 256)), 6)

    def spread_one(level, sources):
        return dot(sources, tables[level])

    def mix_one(level, spread):
        parts = [spread[:, at * 256 : at * 256 + 256] for at in range(terms // QUAD)]
        total = dot(mixers[level - 1], jnp.concatenate(parts, axis=0).astype(BF16))
        fine_step()
        result = jnp.where(quad_lane == 0, total[:8], 0.0)
        for k in range(1, QUAD):
            result = jnp.where(quad_lane == k, total[8 * k : 8 * k + 8], result)
        return result[:, :128] + result[:, 128:]

    coarse_spread = spread_one(2, coarse_sources)
    near_blocks = []
    for d in range(27):
        tile = jnp.where(near_id[d] >= 0, rows[jnp.maximum(near_id[d], 0)].astype(F32), 0.0)
        part = from_coarse[8 * d : 8 * d + 8]
        part = jnp.where((near_code[d] & 2) > 0, part[:, 128:], part[:, :128])
        tile = tile - jnp.where(half_lane == (near_code[d] & 1), part, 0.0)
        near_blocks.append(tile + turn(tile))
    mid_sources = [pair_up(near_blocks[9 * ex : 9 * ex + 9]) for ex in range(3)]
    mid_sources = jnp.concatenate(mid_sources, axis=0).astype(BF16)
    mid_spread = spread_one(1, mid_sources)
    coarse_raw = mix_one(2, coarse_spread)
    tail = dot(stack_halves(coarse_raw), held["coarse_tail"][my_octant & 3])
    fine_step()
    mid_raw = mix_one(1, mid_spread)
    got = tail
    mine = got[:8, :128] + got[:8, 128:256] + got[8:, :128]
    coarse_plane = got[:8, 256:512] + got[:8, 512:] + got[8:, 256:512]
    tail = dot(stack_halves(mid_raw), held["mid_tail"][...])
    from_above = dot(own_out, triple(mine).astype(BF16))
    fine_step()
    got = tail
    mid_plane = got[:8, 128:384] + got[:8, 384:] + got[8:, 128:384]
    planes = jnp.concatenate([triple(j_rows(mid_plane)), triple(j_rows(coarse_plane))], axis=0)
    fine_from = dot(last_matrix, planes.astype(BF16))
    fine_step(3 * terms)
    fine_from = settle(fine_from)
    mid_out = got[:8, :128] + got[8:, :128] + from_above
    for a in range(8):
        at = 64 * (a % 2)
        mid_ref[0:1, 64 * a : 64 * a + 64] = mid_out[a : a + 1, at : at + 64]

    total = sum(fine_total[1:], fine_total[0])
    direct = []
    for a in range(8):
        part = jnp.where(quad_lane == 0, total[8 * a : 8 * a + 8], 0.0)
        for k in range(1, QUAD):
            part = jnp.where(quad_lane == k, total[64 * k + 8 * a : 64 * k + 8 * a + 8], part)
        direct.append(part[:, :128] + part[:, 128:])
    direct = jnp.concatenate(direct, axis=0)
    direct = direct + turn(direct)
    fine_ref[...] = to_flat(live * (direct + fine_from))

    arrived(codes, code_send).wait()
    arrived(rows, row_send).wait()
    for cell in others:
        @pl.when(inside(steps[cell]))
        def _(cell=cell):
            halo_copy(cell).wait_send()


SCALARS = ("mid_child", "mid_parent", "mid_refined", "mid_nbr", "coarse_nbr")


def shards(sizes, fine_coef, mid_leaf, mid_child, mid_parent, mid_refined, fine_nbr, mid_nbr, coarse_nbr,
           op_factor, term_weight):
    levels, terms = op_factor.shape[:2]
    coarse = coarse_nbr.shape[0]
    devices = math.prod(sizes)
    batch = math.gcd(coarse, 4)
    assert mid_child.shape == (1, 8) and fine_coef.shape == (8, 512) and terms % QUAD == 0
    args = dict(
        mid_child=mid_child, mid_parent=mid_parent, mid_refined=mid_refined, fine_coef=fine_coef,
        mid_leaf=mid_leaf, fine_nbr=fine_nbr, mid_nbr=mid_nbr, coarse_nbr=coarse_nbr,
        op_factor=jnp.transpose(op_factor, (0, 2, 3, 4, 1)), term_weight=term_weight[None, :],
    )
    consts = {name: jnp.asarray(value) for name, value in constants(terms, devices, batch).items()}
    arg_names, const_names = list(args), list(consts)
    dma = pltpu.SemaphoreType.DMA
    width = 64 * terms

    def buffer(name, value):
        space = pltpu.SMEM if name in SCALARS else pltpu.VMEM
        return space(value.shape, value.dtype)

    scratch = [buffer(name, value) for name, value in args.items()]
    scratch += [buffer(name, value) for name, value in consts.items()]
    scratch += [
        pltpu.VMEM((27, 8, 512), BF16),
        pltpu.VMEM((devices, 8, 128), BF16),
        pltpu.VMEM((devices, 2, 128), F32),
        pltpu.VMEM((levels * 3, 8, width), F32),
        pltpu.VMEM((levels * 3, 8, width), F32),
        pltpu.VMEM((levels, 576, width), BF16),
        pltpu.VMEM((levels - 1, 8 * QUAD, 24 * (terms // QUAD)), BF16),
        pltpu.VMEM((8 * terms, 192), F32),
        pltpu.VMEM((terms // QUAD // GROUPS, 64 * QUAD, 192 * GROUPS), BF16),
        pltpu.VMEM((192 * (terms // QUAD), 64 * QUAD), BF16),
        pltpu.VMEM((216, 216), BF16),
        pltpu.VMEM((coarse, 8, 128), F32),
        dma((len(args),)), dma((len(consts),)), dma((1,)), dma((1,)), dma((1,)), dma((1,)), dma((27,)), dma((27,)),
    ]

    def body(*refs):
        n_args, n_consts = len(arg_names), len(const_names)
        ins, refs = refs[: n_args + n_consts], refs[n_args + n_consts :]
        outs, refs = refs[:2], refs[2:]
        loaded = dict(zip(arg_names, refs[:n_args]))
        held = dict(zip(const_names, refs[n_args : n_args + n_consts]))
        kernel(sizes, batch, levels, terms, coarse, dict(zip(arg_names, ins[:n_args])),
               dict(zip(const_names, ins[n_args:])), outs, (loaded, held) + tuple(refs[n_args + n_consts :]))

    vmem = pl.BlockSpec(memory_space=pltpu.VMEM)
    hbm = pl.BlockSpec(memory_space=pltpu.HBM)
    shapes = ((8, 512), (1, 512))
    inner = pl.pallas_call(
        body,
        out_shape=tuple(pltpu.VMEM(shape, F32) for shape in shapes),
        in_specs=[hbm] * (len(args) + len(consts)),
        out_specs=(vmem, vmem),
        scratch_shapes=scratch,
        compiler_params=pltpu.CompilerParams(
            collective_id=0, has_side_effects=True, vmem_limit_bytes=58 * 1024 * 1024),
        name="tree",
    )(*args.values(), *consts.values())

    def store(fine_in, mid_in, fine_to, mid_to, sem):
        copies = [
            pltpu.make_async_copy(fine_in, fine_to, sem.at[0]),
            pltpu.make_async_copy(mid_in, mid_to, sem.at[1]),
        ]
        for copy in copies:
            copy.start()
        for copy in copies:
            copy.wait()

    return pl.pallas_call(
        store,
        out_shape=tuple(jax.ShapeDtypeStruct(shape, F32) for shape in shapes),
        in_specs=[pl.BlockSpec(memory_space=pl.ANY)] * 2,
        out_specs=(hbm, hbm),
        scratch_shapes=[dma((2,))],
        compiler_params=pltpu.CompilerParams(vmem_limit_bytes=1 << 20),
        name="store",
    )(*inner)


def solution(mesh):
    sizes = tuple(mesh.shape[axis] for axis in AXES)
    split = P(AXES, None)
    line = P(AXES)
    return jax.shard_map(
        lambda *args: shards(sizes, *args),
        mesh=mesh,
        in_specs=(split, split, split, line, line, split, split, P(), P(), P()),
        out_specs=(split, split),
        check_vma=False,
    )
```

```python
import math

import jax
import jax.numpy as jnp
import numpy as np
from jax import lax
from jax.experimental import pallas as pl
from jax.experimental.pallas import tpu as pltpu
from jax.sharding import PartitionSpec as P

MESH = pl.DeviceIdType.MESH
AXES = ("gx", "gy", "gz")
CENTRE = 13
QUAD = 4
EARLY = 1
GROUPS = 4
F32 = jnp.float32
BF16 = jnp.bfloat16


def poly_multiply(left, right):
    result = [0.0] * (len(left) + len(right) - 1)
    for first, left_coef in enumerate(left):
        for second, right_coef in enumerate(right):
            result[first + second] += left_coef * right_coef
    return result


def poly_compose(coeffs, factor, offset):
    result = [0.0]
    power_term = [1.0]
    for coef in coeffs:
        padded = result + [0.0] * (len(power_term) - len(result))
        result = [padded[place] + coef * power_term[place] for place in range(len(power_term))]
        power_term = poly_multiply(power_term, [offset, factor])
    return result


def legendre_table(basis_order):
    polys = [[1.0], [0.0, 1.0]]
    for degree in range(1, basis_order):
        upper = [0.0] + [(2 * degree + 1) * coef for coef in polys[degree]]
        lower = [degree * coef for coef in polys[degree - 1]] + [0.0] * (
            len(upper) - len(polys[degree - 1])
        )
        polys.append([(upper[place] - lower[place]) / (degree + 1) for place in range(len(upper))])
    return [
        [math.sqrt(2 * degree + 1) * coef for coef in poly_compose(polys[degree], 2.0, -1.0)]
        for degree in range(basis_order)
    ]


def two_scale(basis_order):
    shifted = legendre_table(basis_order)
    filters = np.zeros((2, basis_order, basis_order))
    for which_half in range(2):
        for row_at in range(basis_order):
            halved = poly_compose(shifted[row_at], 0.5, 0.5 * which_half)
            for col_at in range(basis_order):
                product = poly_multiply(halved, shifted[col_at])
                total = sum((coef / (place + 1) for place, coef in enumerate(product)))
                filters[which_half, row_at, col_at] = total / math.sqrt(2.0)
    return np.asarray(filters, np.float32)


def halves(array):
    high = array.astype(BF16)
    return high, (array - high.astype(array.dtype)).astype(BF16)


def np_halves(array):
    array = np.asarray(array, np.float32)
    high = array.astype(BF16)
    return high, (array - high.astype(np.float32)).astype(BF16)


def dot(left, right):
    return jnp.dot(left, right, preferred_element_type=F32)


def dot_rows(left, right):
    return lax.dot_general(left, right, (((1,), (1,)), ((), ())), preferred_element_type=F32)


def constants(terms, devices, batch):
    filters = two_scale(8)
    exact = np.asarray(filters, np.float64)
    table = {}
    row = np.arange(8 * terms)
    lane = np.arange(64 * QUAD)
    same = (row % terms)[:, None] == (lane // 64)[None, :]
    spread = [same & ((row // terms)[:, None] == part[None, :]) for part in (lane // 8 % 8, lane % 8)]
    table["spread"] = np.concatenate(spread, axis=1).astype(BF16)
    swap = (row // 8)[:, None] == (row % terms)[None, :]
    swap &= (row % 8)[:, None] == (row // terms)[None, :]
    table["swap"] = swap.astype(BF16)
    table["widen"] = (np.arange(72)[:, None] == (np.arange(192) // 8)[None, :]).astype(BF16)
    close = np.einsum("jqy,lrz->jlyzqr", exact, exact).reshape(256, 64)
    opened = np.ascontiguousarray(close.T)
    twice = np.concatenate([close, close], axis=1)
    table["close"] = np.concatenate(np_halves(twice), axis=1)
    table["open"] = np.concatenate([np.concatenate(np_halves(opened), axis=1)] * 2, axis=0)
    table["coarse"] = np.concatenate(np_halves(twice) + np_halves(close @ opened), axis=1)
    fold = np.tile(np.eye(64, dtype=np.float32), (2, 2)).astype(BF16)
    stack = np.tile(opened, (2, 1))
    table["mid_tail"] = np.concatenate((fold,) + np_halves(stack), axis=1)
    tails = []
    for jl in range(4):
        mine = opened[:, 64 * jl : 64 * jl + 64]
        both = np.tile(np.concatenate([mine, mine], axis=1), (2, 1))
        tails.append(np.concatenate(np_halves(both) + np_halves(np.tile(mine @ opened, (2, 1))), axis=1))
    table["coarse_tail"] = np.stack(tails)
    parts = [np.asarray(part, np.float32) for part in np_halves(filters)]
    both = np.stack(parts, axis=1).reshape(4, 8, 8)
    flip = np.swapaxes(both, 1, 2)
    table["child_in"] = np.repeat(both, 8, axis=2)
    chains = [[exact[i].T for i in range(2)]]
    chains += [[exact[i].T @ exact[own].T for i in range(2)] for own in range(2)]
    out = np.stack([np.stack(np_halves(chain)) for chain_set in chains for chain in chain_set])
    out = np.asarray(out, np.float32).reshape(12, 8, 8)
    table["child_out"] = np.tile(np.repeat(out, 8, axis=1), (1, 1, 2))
    table["mid_in"] = np.tile(both, (1, 1, devices))
    table["mid_out"] = np.tile(flip, (1, 1, batch))
    own = [np.concatenate([flip[2 * i], flip[2 * i], flip[2 * i + 1]], axis=1) for i in range(2)]
    table["own_out"] = np.stack(own)
    cell = np.arange(27 * 8) // 8
    cells = np.zeros((8, 27 * 8), np.int32)
    cells[:4] = np.stack([cell // 9 - 1, cell // 3 % 3 - 1, cell % 3 - 1, np.arange(27 * 8) % 8])
    table["cells"] = cells
    return table


def kernel(sizes, batch, levels, terms, coarse, args, consts, outs, scratch):
    size_x, size_y, size_z = sizes
    devices = size_x * size_y * size_z
    here = [lax.axis_index(axis) for axis in AXES]
    me = (here[0] * size_y + here[1]) * size_z + here[2]
    fine_ref, mid_ref = outs
    (loaded, held, halo, rows, codes, factor_left, factor_right, tables, mixers, mixers_t, block_mix, spreads, picks,
     coarse_tab, load_sem, held_sem, row_send, row_recv, code_send, code_recv, halo_send, halo_recv) = scratch

    spots = [(x, y, z) for x in range(size_x) for y in range(size_y) for z in range(size_z)]
    spots.sort(key=lambda spot: spot[0] // 2 + spot[1] + spot[2])
    front = [spot for spot in spots if spot[0] // 2 + spot[1] + spot[2] <= 0]
    unrolled = devices <= 64

    def each_peer(body, chosen=spots):
        if unrolled:
            for spot in chosen:
                @pl.when(me != (spot[0] * size_y + spot[1]) * size_z + spot[2])
                def _(spot=spot):
                    body(spot)
        else:
            def step(offset, carry):
                device = lax.rem(me + offset, devices)
                body((device // (size_y * size_z), device // size_z % size_y, device % size_z))
                return carry
            lax.fori_loop(1, devices, step, 0)

    loads = {}
    for at, (name, source) in enumerate(args.items()):
        loads[name] = pltpu.make_async_copy(source, loaded[name], load_sem.at[at])
    for at, (name, source) in enumerate(consts.items()):
        loads[name] = pltpu.make_async_copy(source, held[name], held_sem.at[at])
    order = ["mid_child", "mid_parent", "mid_refined", "fine_coef", "mid_leaf", "child_in", "close",
             "child_out", "open"]
    order += [name for name in loads if name not in order]
    for name in order[:9]:
        loads[name].start()
    barrier = pltpu.get_barrier_semaphore()
    each_peer(lambda peer: pl.semaphore_signal(
        barrier, inc=1, device_id=peer, device_id_type=MESH))
    for name in order[9:]:
        loads[name].start()

    def ready(*wanted):
        for name in wanted:
            loads[name].wait()

    def turn(array):
        return pltpu.roll(array, 64, 1)

    def lanes(shape):
        return lax.broadcasted_iota(jnp.int32, shape, len(shape) - 1)

    def stack_halves(array):
        high, low = halves(array)
        return jnp.concatenate([high.astype(F32), low.astype(F32)], axis=0).astype(BF16)

    def triple(array):
        high, low = halves(array)
        high, low = high.astype(F32), low.astype(F32)
        return jnp.concatenate([high, low, high], axis=0)

    half_lane = lax.shift_right_logical(lanes((8, 128)), 6)
    low_lane = half_lane == 0

    ready("mid_child", "mid_parent", "mid_refined", "fine_coef", "mid_leaf", "child_in", "close")
    child = [loaded["mid_child"][0, o] for o in range(8)]
    refined = loaded["mid_refined"][0] > 0
    live = jnp.where(refined, 1.0, 0.0).astype(F32)
    mid_parent = loaded["mid_parent"][0]
    my_parent = lax.shift_right_logical(mid_parent, 3)
    my_octant = mid_parent & 7
    code_lane = lax.shift_right_logical(lanes((1, 128)), 3) == (me & 15)
    codes[me] = jnp.where(code_lane, mid_parent + 1, 0).astype(F32)

    flat = loaded["fine_coef"][...].astype(F32)
    by_row = []
    for k in range(4):
        tile = flat[:, 128 * k : 128 * k + 128]
        turned = turn(tile)
        by_row += [jnp.where(low_lane, tile, turned), jnp.where(low_lane, turned, tile)]
    by_row = jnp.concatenate(by_row, axis=0)
    slot_lane = lanes((8, 64)) & 7
    child_in = [held["child_in"][k] for k in range(4)]
    blocks = []
    for part in range(2):
        for jl in range(4):
            block = jnp.where(slot_lane == child[jl], child_in[part], 0.0)
            blocks.append(block + jnp.where(slot_lane == child[4 + jl], child_in[2 + part], 0.0))
    mixed = dot(jnp.concatenate(blocks, axis=0).astype(BF16), by_row.astype(BF16))
    mixed = mixed[:32] + mixed[32:]
    wide = [jnp.where(low_lane, mixed[16 * j : 16 * j + 8], mixed[16 * j + 8 : 16 * j + 16]) for j in range(2)]
    got = dot(stack_halves(jnp.concatenate(wide, axis=1)), held["close"][...])
    compressed = got[:8, :128] + got[:8, 128:] + got[8:, :128]
    leaf = jnp.broadcast_to(loaded["mid_leaf"][...].astype(F32), (8, 512))
    leaf_block = lax.shift_right_logical(lanes((8, 512)), 6)
    leaf = jnp.where(leaf_block == lax.broadcasted_iota(jnp.int32, (8, 512), 0), leaf, 0.0)
    leaf = leaf[:, :128] + leaf[:, 128:256] + leaf[:, 256:384] + leaf[:, 384:]
    leaf = leaf + turn(leaf)
    mid_source = jnp.where(refined, compressed, leaf)
    placed = jnp.where(half_lane == (my_octant & 1), mid_source, 0.0).astype(BF16)
    rows[me] = placed

    ready("child_out", "open")
    j_lane = lax.shift_right_logical(lanes((64, 16)), 3)
    slot_row = lax.broadcasted_iota(jnp.int32, (64, 16), 0) & 7
    chosen = []
    for i in range(2):
        ends = [jnp.where(j_lane == 0, child[4 * i + l], child[4 * i + 2 + l]) for l in range(2)]
        chosen.append((slot_row == ends[0]) | (slot_row == ends[1]))

    def child_matrix(at):
        parts = [
            jnp.where(chosen[0], held["child_out"][4 * at + part], 0.0)
            + jnp.where(chosen[1], held["child_out"][4 * at + 2 + part], 0.0)
            for part in range(2)
        ]
        return [parts[0], parts[0], parts[1]]

    odd = lax.broadcasted_iota(jnp.int32, (8, 128), 0)
    odd = (odd == child[1]) | (odd == child[3]) | (odd == child[5]) | (odd == child[7])
    child_half = jnp.concatenate([odd == (half_lane == 1)] * 8, axis=0)

    def j_rows(plane):
        return jnp.concatenate([plane[:, :128], plane[:, 128:]], axis=0)

    def settle(array):
        array = jnp.where(child_half, array, 0.0)
        return array + turn(array)

    def to_flat(array):
        pairs = [jnp.where(low_lane, array[16 * k : 16 * k + 8], array[16 * k + 8 : 16 * k + 16]) for k in range(4)]
        return jnp.concatenate(pairs, axis=1)

    steps = [(c // 9 - 1, c // 3 % 3 - 1, c % 3 - 1) for c in range(27)]

    def inside(step):
        tests = []
        for at, size, move in zip(here, sizes, step):
            if move == 1:
                tests.append(at < size - 1)
            elif move == -1:
                tests.append(at > 0)
        found = tests[0]
        for test in tests[1:]:
            found = found & test
        return found

    def halo_copy(cell):
        peer = tuple(at + part for at, part in zip(here, steps[cell]))
        return pltpu.make_async_remote_copy(
            src_ref=halo.at[CENTRE],
            dst_ref=halo.at[26 - cell],
            send_sem=halo_send.at[cell],
            recv_sem=halo_recv.at[26 - cell],
            device_id=peer,
            device_id_type=MESH,
        )

    def send_code(peer):
        pltpu.make_async_remote_copy(
            src_ref=codes.at[me],
            dst_ref=codes.at[me],
            send_sem=code_send.at[0],
            recv_sem=code_recv.at[0],
            device_id=peer,
            device_id_type=MESH,
        ).start()

    def send_row(peer):
        pltpu.make_async_remote_copy(
            src_ref=rows.at[me],
            dst_ref=rows.at[me],
            send_sem=row_send.at[0],
            recv_sem=row_recv.at[0],
            device_id=peer,
            device_id_type=MESH,
        ).start()

    def send_both(peer):
        send_code(peer)
        send_row(peer)

    others = [cell for cell in range(27) if cell != CENTRE]

    def meet_and_send():
        pl.semaphore_wait(barrier, devices - 1)
        if unrolled:
            each_peer(send_both, front)
            each_peer(send_code, spots[len(front) :])
            each_peer(send_row, spots[len(front) :])
        else:
            each_peer(send_both)

    def build_tables():
        ready("op_factor", "term_weight", "spread", "swap", "widen")
        factor = loaded["op_factor"]
        planes = []
        for level in range(levels):
            for e in range(3):
                planes.append(jnp.concatenate([factor[level, e, b] for b in range(8)], axis=1))
        plane = jnp.concatenate(planes, axis=0)
        weight = jnp.concatenate([loaded["term_weight"][...]] * 8, axis=1)
        rounded = plane.astype(BF16)
        left_side = stack_halves(plane * weight).astype(F32)
        right_side = stack_halves(plane).astype(F32)
        count = plane.shape[0]
        group = 64 * QUAD
        for at in range(terms // QUAD):
            for side, first, factors in ((left_side, 0, factor_left), (right_side, group, factor_right)):
                some = pltpu.roll(side, 8 * terms - QUAD * at, 1) if at else side
                got = dot(some.astype(BF16), held["spread"][:, first : first + group])
                got = got[:count] + got[count:]
                factors[:, :, at * group : at * group + group] = got.reshape(levels * 3, 8, group)
        turned = dot_rows(held["swap"][...], rounded)
        for level in range(1, levels):
            parts = [turned[32 * at : 32 * at + 32, 24 * level : 24 * level + 24] for at in range(terms // QUAD)]
            mixers[level - 1] = jnp.concatenate(parts, axis=1).astype(BF16)
        mixers_t[...] = dot(turned.astype(BF16), held["widen"][...])

        def table_step(at, carry):
            level, ey = at // 3, at % 3
            left = factor_left.at[at]
            for ez in range(3):
                right = factor_right[level * 3 + ez]
                base = (ey * 3 + ez) * 64
                for k in range(4):
                    pair = [left[2 * k + half : 2 * k + half + 1, :] * right for half in range(2)]
                    start = pl.multiple_of(base + 16 * k, 16)
                    tables[level, pl.ds(start, 16), :] = jnp.concatenate(pair, axis=0).astype(BF16)
            return carry

        lax.fori_loop(0, levels * 3, table_step, 0)
        own_lane = (lanes((8, 192)) & 7) == lax.broadcasted_iota(jnp.int32, (8, 192), 0)

        for at in range(terms // 2):
            some = mixers_t[16 * at : 16 * at + 16, :]
            some = jnp.where(own_lane[None], jnp.broadcast_to(some[:, None, :], (16, 8, 192)), 0.0)
            part, first, lane = at // (2 * GROUPS), 128 * (at % 2), 192 * (at // 2 % GROUPS)
            block_mix[part, first : first + 128, lane : lane + 192] = some.reshape(128, 192).astype(BF16)

    away = lax.shift_right_logical(here[0], 1) + here[1] + here[2]
    far = 2 * away > (size_x - 1) // 2 + size_y + size_z - 2
    near_start = away <= EARLY

    @pl.when(far)
    def _():
        meet_and_send()

    own_matrix = child_matrix(0)
    plane = dot(placed, held["open"][...])
    plane = plane[:, :256] + plane[:, 256:]
    fine_from = dot(jnp.concatenate(own_matrix, axis=1).astype(BF16), triple(j_rows(plane)).astype(BF16))
    detail = live * (by_row - settle(fine_from))
    halo[CENTRE] = to_flat(detail).astype(BF16)

    for cell in others:
        @pl.when(jnp.logical_not(inside(steps[cell])))
        def _(cell=cell):
            halo[cell] = jnp.zeros(halo.shape[1:], BF16)

    @pl.when(near_start)
    def _():
        build_tables()

    @pl.when(jnp.logical_not(far))
    def _():
        meet_and_send()

    for cell in others:
        @pl.when(inside(steps[cell]))
        def _(cell=cell):
            halo_copy(cell).start()

    @pl.when(jnp.logical_not(near_start))
    def _():
        build_tables()

    ready("cells", "fine_nbr")
    cells = held["cells"]
    spot = [here[k] + cells[k : k + 1, :] for k in range(3)]
    there = None
    for k in range(3):
        test = (spot[k] >= 0) & (spot[k] < sizes[k])
        there = test if there is None else there & test
    names_row = ((spot[0] * size_y + spot[1]) * size_z + spot[2]) * 8 + cells[3:4, :]
    names_row = jnp.where(there, names_row, -2)
    near = loaded["fine_nbr"][...]
    hot = [(near[:, d : d + 1] == names_row).astype(F32) for d in range(27)]
    picks[...] = jnp.concatenate(hot, axis=0).astype(BF16)

    ready("mid_in", "mid_out", "own_out", "mid_nbr", "coarse_nbr", "coarse", "mid_tail", "coarse_tail")
    after_matrix = [jnp.where(my_octant >= 4, upper, lower)
                    for lower, upper in zip(child_matrix(1), child_matrix(2))]
    last_matrix = jnp.concatenate(own_matrix + after_matrix, axis=1).astype(BF16)
    own_out = jnp.where(my_octant >= 4, held["own_out"][1], held["own_out"][0]).astype(BF16)

    def arrived(buffer, sem):
        span = buffer.at[pl.ds(0, devices - 1)]
        return pltpu.make_async_copy(span, span, sem.at[0])

    arrived(codes, code_recv).wait()
    code = [
        jnp.sum(codes[first : min(first + 16, devices)], axis=0) for first in range(0, devices, 16)
    ]
    code = jnp.concatenate(code, axis=1)[:, : devices * 8].astype(jnp.int32) - 1
    key = lax.shift_right_arithmetic(jnp.broadcast_to(code, (8, devices * 8)), 1)
    near_id = [loaded["mid_nbr"][0, d] for d in range(27)]
    near_code = []
    for named in near_id:
        got = jnp.max(codes[jnp.maximum(named, 0)], axis=1, keepdims=True).astype(jnp.int32)
        near_code.append(jnp.broadcast_to(jnp.where(named >= 0, got, 0) - 1, (8, 128)))
    batch_lane = lax.shift_right_logical(lanes((8, batch * 8)), 3)

    def choose_in(first):
        blocks = []
        for part in range(2):
            for k in range(batch):
                for j in range(2):
                    want = (first + k) * 4 + j
                    block = jnp.where(key == want, held["mid_in"][part], 0.0)
                    blocks.append(block + jnp.where(key == want + 2, held["mid_in"][2 + part], 0.0))
        return jnp.concatenate(blocks, axis=0).astype(BF16)

    def choose_out(first):
        lane_key = (first + batch_lane) * 2
        parts = [[], []]
        for d in range(27):
            mine = lax.shift_right_arithmetic(near_code[d][:, : batch * 8], 2)
            lower, upper = mine == lane_key, mine == lane_key + 1
            for part in range(2):
                block = jnp.where(lower, held["mid_out"][part], 0.0)
                parts[part].append(block + jnp.where(upper, held["mid_out"][2 + part], 0.0))
        parts = [jnp.concatenate(part, axis=0) for part in parts]
        return jnp.concatenate([parts[0], parts[0], parts[1]], axis=1).astype(BF16)

    batches = coarse // batch
    if batches == 1:
        first_in, first_out = choose_in(0), choose_out(0)

    for cell in others:
        @pl.when(inside(steps[cell]))
        def _(cell=cell):
            halo_copy(26 - cell).wait_recv()
    got = dot(picks[...], halo[...].astype(F32).reshape(216, 512).astype(BF16))
    blocks = []
    for ex in range(3):
        here_rows = [got[(ex * 9 + e) * 8 : (ex * 9 + e) * 8 + 8] for e in range(9)]
        for k in range(4):
            tile = [part[:, 128 * k : 128 * k + 128] for part in here_rows]
            turned = [turn(part) for part in tile]
            even = [jnp.where(low_lane, tile[e], turned[e + 1]) for e in range(0, 8, 2)]
            uneven = [jnp.where(low_lane, turned[e], tile[e + 1]) for e in range(0, 8, 2)]
            blocks.append(jnp.concatenate(even + [tile[8][:, :64]], axis=1))
            blocks.append(jnp.concatenate(uneven + [turned[8][:, :64]], axis=1))
    fine_sources = jnp.concatenate(blocks, axis=0).astype(BF16)
    fine_total = []

    def spread_fine(at):
        spread = dot(fine_sources, tables[0, :, at * 256 : at * 256 + 256])
        spreads[192 * at : 192 * at + 192, :] = spread.astype(BF16)

    def mix_fine(part):
        rows_of = 192 * GROUPS
        fine_total.append(dot(block_mix[part], spreads[rows_of * part : rows_of * part + rows_of, :]))

    fine_work = []
    for at in range(terms // QUAD):
        fine_work.append(lambda at=at: spread_fine(at))
        if at >= GROUPS and at % GROUPS == 0:
            fine_work.append(lambda part=at // GROUPS - 1: mix_fine(part))
    fine_work.append(lambda: mix_fine(terms // QUAD // GROUPS - 1))
    fine_work = iter(fine_work)

    def fine_step(count=1):
        for _, work in zip(range(count), fine_work):
            work()

    arrived(rows, row_recv).wait()
    gathered = rows[...].astype(F32).reshape(devices * 8, 128).astype(BF16)

    def coarse_step(at, total, chosen_in, chosen_out, between=lambda: None):
        mixed = dot(chosen_in, gathered)
        between()
        mixed = mixed[: batch * 16] + mixed[batch * 16 :]
        wide = [
            jnp.concatenate([mixed[16 * k : 16 * k + 8], mixed[16 * k + 8 : 16 * k + 16]], axis=1)
            for k in range(batch)
        ]
        got = dot(stack_halves(jnp.concatenate(wide, axis=0)), held["coarse"][...])
        between()
        top = batch * 8
        plane = got[:top, 256:512] + got[:top, 512:] + got[top:, 256:512]
        source = got[:top, :128] + got[:top, 128:256] + got[top:, :128]
        coarse_tab[pl.ds(at * batch, batch)] = source.reshape(batch, 8, 128)
        found = dot(chosen_out, triple(plane).astype(BF16))
        return found if total is None else total + found

    zero = jnp.zeros((216, 256), F32)
    if batches == 1:
        from_coarse = coarse_step(0, None, first_in, first_out, fine_step)
    else:
        from_coarse = lax.fori_loop(
            0, batches,
            lambda at, total: coarse_step(at, total, choose_in(at * batch), choose_out(at * batch)), zero)

    def pair_up(blocks):
        pairs = [jnp.where(low_lane, blocks[e], blocks[e + 1]) for e in range(0, 8, 2)]
        return jnp.concatenate(pairs + [blocks[8][:, :64]], axis=1)

    coarse_blocks = []
    for ex in range(3):
        got = []
        for e in range(9):
            named = loaded["coarse_nbr"][my_parent, ex * 9 + e]
            got.append(jnp.where(named >= 0, coarse_tab[jnp.maximum(named, 0)], 0.0))
        coarse_blocks.append(pair_up(got))
    coarse_sources = jnp.concatenate(coarse_blocks, axis=0).astype(BF16)
    quad_lane = lax.shift_right_logical(lanes((8, 256)), 6)

    def spread_one(level, sources):
        return dot(sources, tables[level])

    def mix_one(level, spread):
        parts = [spread[:, at * 256 : at * 256 + 256] for at in range(terms // QUAD)]
        total = dot(mixers[level - 1], jnp.concatenate(parts, axis=0).astype(BF16))
        fine_step()
        result = jnp.where(quad_lane == 0, total[:8], 0.0)
        for k in range(1, QUAD):
            result = jnp.where(quad_lane == k, total[8 * k : 8 * k + 8], result)
        return result[:, :128] + result[:, 128:]

    coarse_spread = spread_one(2, coarse_sources)
    near_blocks = []
    for d in range(27):
        tile = jnp.where(near_id[d] >= 0, rows[jnp.maximum(near_id[d], 0)].astype(F32), 0.0)
        part = from_coarse[8 * d : 8 * d + 8]
        part = jnp.where((near_code[d] & 2) > 0, part[:, 128:], part[:, :128])
        tile = tile - jnp.where(half_lane == (near_code[d] & 1), part, 0.0)
        near_blocks.append(tile + turn(tile))
    mid_sources = [pair_up(near_blocks[9 * ex : 9 * ex + 9]) for ex in range(3)]
    mid_sources = jnp.concatenate(mid_sources, axis=0).astype(BF16)
    mid_spread = spread_one(1, mid_sources)
    coarse_raw = mix_one(2, coarse_spread)
    tail = dot(stack_halves(coarse_raw), held["coarse_tail"][my_octant & 3])
    fine_step()
    mid_raw = mix_one(1, mid_spread)
    got = tail
    mine = got[:8, :128] + got[:8, 128:256] + got[8:, :128]
    coarse_plane = got[:8, 256:512] + got[:8, 512:] + got[8:, 256:512]
    tail = dot(stack_halves(mid_raw), held["mid_tail"][...])
    from_above = dot(own_out, triple(mine).astype(BF16))
    fine_step()
    got = tail
    mid_plane = got[:8, 128:384] + got[:8, 384:] + got[8:, 128:384]
    planes = jnp.concatenate([triple(j_rows(mid_plane)), triple(j_rows(coarse_plane))], axis=0)
    fine_from = dot(last_matrix, planes.astype(BF16))
    fine_step(3 * terms)
    fine_from = settle(fine_from)
    mid_out = got[:8, :128] + got[8:, :128] + from_above
    for a in range(8):
        at = 64 * (a % 2)
        mid_ref[0:1, 64 * a : 64 * a + 64] = mid_out[a : a + 1, at : at + 64]

    total = sum(fine_total[1:], fine_total[0])
    direct = []
    for a in range(8):
        part = jnp.where(quad_lane == 0, total[8 * a : 8 * a + 8], 0.0)
        for k in range(1, QUAD):
            part = jnp.where(quad_lane == k, total[64 * k + 8 * a : 64 * k + 8 * a + 8], part)
        direct.append(part[:, :128] + part[:, 128:])
    direct = jnp.concatenate(direct, axis=0)
    direct = direct + turn(direct)
    fine_ref[...] = to_flat(live * (direct + fine_from))

    arrived(codes, code_send).wait()
    arrived(rows, row_send).wait()
    for cell in others:
        @pl.when(inside(steps[cell]))
        def _(cell=cell):
            halo_copy(cell).wait_send()


SCALARS = ("mid_child", "mid_parent", "mid_refined", "mid_nbr", "coarse_nbr")


def shards(sizes, fine_coef, mid_leaf, mid_child, mid_parent, mid_refined, fine_nbr, mid_nbr, coarse_nbr,
           op_factor, term_weight):
    levels, terms = op_factor.shape[:2]
    coarse = coarse_nbr.shape[0]
    devices = math.prod(sizes)
    batch = math.gcd(coarse, 4)
    assert mid_child.shape == (1, 8) and fine_coef.shape == (8, 512) and terms % QUAD == 0
    args = dict(
        mid_child=mid_child, mid_parent=mid_parent, mid_refined=mid_refined, fine_coef=fine_coef,
        mid_leaf=mid_leaf, fine_nbr=fine_nbr, mid_nbr=mid_nbr, coarse_nbr=coarse_nbr,
        op_factor=jnp.transpose(op_factor, (0, 2, 3, 4, 1)), term_weight=term_weight[None, :],
    )
    consts = {name: jnp.asarray(value) for name, value in constants(terms, devices, batch).items()}
    arg_names, const_names = list(args), list(consts)
    dma = pltpu.SemaphoreType.DMA
    width = 64 * terms

    def buffer(name, value):
        space = pltpu.SMEM if name in SCALARS else pltpu.VMEM
        return space(value.shape, value.dtype)

    scratch = [buffer(name, value) for name, value in args.items()]
    scratch += [buffer(name, value) for name, value in consts.items()]
    scratch += [
        pltpu.VMEM((27, 8, 512), BF16),
        pltpu.VMEM((devices, 8, 128), BF16),
        pltpu.VMEM((devices, 1, 128), F32),
        pltpu.VMEM((levels * 3, 8, width), F32),
        pltpu.VMEM((levels * 3, 8, width), F32),
        pltpu.VMEM((levels, 576, width), BF16),
        pltpu.VMEM((levels - 1, 8 * QUAD, 24 * (terms // QUAD)), BF16),
        pltpu.VMEM((8 * terms, 192), F32),
        pltpu.VMEM((terms // QUAD // GROUPS, 64 * QUAD, 192 * GROUPS), BF16),
        pltpu.VMEM((192 * (terms // QUAD), 64 * QUAD), BF16),
        pltpu.VMEM((216, 216), BF16),
        pltpu.VMEM((coarse, 8, 128), F32),
        dma((len(args),)), dma((len(consts),)), dma((1,)), dma((1,)), dma((1,)), dma((1,)), dma((27,)), dma((27,)),
    ]

    def body(*refs):
        n_args, n_consts = len(arg_names), len(const_names)
        ins, refs = refs[: n_args + n_consts], refs[n_args + n_consts :]
        outs, refs = refs[:2], refs[2:]
        loaded = dict(zip(arg_names, refs[:n_args]))
        held = dict(zip(const_names, refs[n_args : n_args + n_consts]))
        kernel(sizes, batch, levels, terms, coarse, dict(zip(arg_names, ins[:n_args])),
               dict(zip(const_names, ins[n_args:])), outs, (loaded, held) + tuple(refs[n_args + n_consts :]))

    vmem = pl.BlockSpec(memory_space=pltpu.VMEM)
    hbm = pl.BlockSpec(memory_space=pltpu.HBM)
    shapes = ((8, 512), (1, 512))
    inner = pl.pallas_call(
        body,
        out_shape=tuple(pltpu.VMEM(shape, F32) for shape in shapes),
        in_specs=[hbm] * (len(args) + len(consts)),
        out_specs=(vmem, vmem),
        scratch_shapes=scratch,
        compiler_params=pltpu.CompilerParams(
            collective_id=0, has_side_effects=True, vmem_limit_bytes=58 * 1024 * 1024),
        name="tree",
    )(*args.values(), *consts.values())

    def store(fine_in, mid_in, fine_to, mid_to, sem):
        copies = [
            pltpu.make_async_copy(fine_in, fine_to, sem.at[0]),
            pltpu.make_async_copy(mid_in, mid_to, sem.at[1]),
        ]
        for copy in copies:
            copy.start()
        for copy in copies:
            copy.wait()

    return pl.pallas_call(
        store,
        out_shape=tuple(jax.ShapeDtypeStruct(shape, F32) for shape in shapes),
        in_specs=[pl.BlockSpec(memory_space=pl.ANY)] * 2,
        out_specs=(hbm, hbm),
        scratch_shapes=[dma((2,))],
        compiler_params=pltpu.CompilerParams(vmem_limit_bytes=1 << 20),
        name="store",
    )(*inner)


def solution(mesh):
    sizes = tuple(mesh.shape[axis] for axis in AXES)
    split = P(AXES, None)
    line = P(AXES)
    return jax.shard_map(
        lambda *args: shards(sizes, *args),
        mesh=mesh,
        in_specs=(split, split, split, line, line, split, split, P(), P(), P()),
        out_specs=(split, split),
        check_vma=False,
    )
```
